32 devices in a mesh: ep: 16 (over z, y, x), dp: 2 (over core).
Axes of the slice: x: 2, y: 2, z: 4, core: 2. Of those that a mesh axis runs over, the one named last changes fastest.
Arguments:
- layer_input: bfloat16 [2048, 3584], P('ep'), may hold values from -6 to 6
- out_grad: bfloat16 [2048, 3584], P('ep'), may hold values from -6 to 6
- expert_ids: int32 [2048, 8], P('ep'), may hold values from 0 to 15, all different within a row; in each aligned block of 128 rows (0 to 127, 128 to 255, ...) at most 80 rows name the same one
- gate_probs: float32 [2048, 8], P('ep'), may hold values from 0.1 to 1
- gate_proj: bfloat16 [16, 3584, 1024], P('ep'), may hold values from -0.09375 to 0.09375
- up_proj: bfloat16 [16, 3584, 1024], P('ep'), may hold values from -0.09375 to 0.09375
- down_proj: bfloat16 [16, 1024, 3584], P('ep'), may hold values from -0.1875 to 0.1875
Outputs:
- input_grad: bfloat16 [2048, 3584], P('ep', 'dp')
The draws below stay inside these ranges and needn't reach their ends.
Inputs may be any that keep to these rules, and one draw needn't show every extreme that they name: `expert_ids`: each row names 8 different experts. The 128 rows of one device name one expert at most 80 times, and in every draw some device's rows name some expert exactly 80 times.
All inputs are finite; a program needn't handle non-finite values.
Results may differ from the reference program's by a relative error of at most 0.0058.
Values may be sent and summed in bfloat16 or wider, within the bound.
A program may use at most 192 MiB of HBM per device.

```python
import math
import jax
import jax.numpy as jnp
import numpy as np
from jax import lax

D = 3584
FF = 1024
TOP = 8
TOK_DEV = 128
EXPERTS = 16
CAP = 80
TOKENS = 2048
N_EP = 16


def level_of(rng, extent, shards, least, high):
    gain, own = 1.0, jax.random.fold_in(rng, 6)
    for dim, parts in shards:
        heights = jnp.exp(jax.random.uniform(jax.random.fold_in(own, dim), (parts,), jnp.float32, least / len(shards), high / len(shards)))
        gain = gain * jnp.repeat(heights, extent[dim] // parts).reshape([-1 if axis == dim else 1 for axis in range(len(extent))])
    return gain


def assign_block(rng, own, number, rows, amount, top, limit, lean):
    order = jax.random.permutation(rng, amount)
    packed, usual = portions_of(amount, rows * top, limit, lean, True), portions_of(amount, rows * top, limit, lean, False)
    places = jnp.arange(amount)

    def named(sizes, turn):
        used = int((sizes > 0).sum())
        fixed = max(1, used // 4)
        moved = fixed + (places - fixed + turn * (used - fixed)) % max(1, amount - fixed)
        return jnp.zeros((amount,), jnp.int32).at[order[jnp.where(places < fixed, places, moved)]].set(jnp.asarray(sizes, jnp.int32))

    sizes = jnp.where(number % 4 == 0, named(packed, number // 4), named(usual, number - number // 4 - 1))
    mixed = jax.random.permutation(jax.random.fold_in(own, 3), amount)
    donor, sink = mixed[0:amount // 2 * 2:2], mixed[1:amount // 2 * 2:2]
    room = jnp.minimum(sizes[donor] - 1, limit - sizes[sink]) // 2
    room = jnp.where((donor == order[0]) | (sink == order[0]) | (sizes[sink] == 0), 0, jnp.maximum(room, 0))
    moved = jax.random.randint(jax.random.fold_in(own, 4), (amount // 2,), 0, 1 << 20) % (room + 1)
    sizes = sizes.at[donor].add(-moved).at[sink].add(moved)
    labels = jnp.searchsorted(jnp.cumsum(sizes), jnp.arange(rows * top), side="right").astype(jnp.int32)
    listing = labels.reshape(top, rows).T
    listing = listing[jax.random.permutation(jax.random.fold_in(own, 1), rows)]
    turn = jax.random.randint(jax.random.fold_in(own, 2), (rows, 1), 0, top)
    return jnp.take_along_axis(listing, (jnp.arange(top)[None, :] + turn) % top, axis=1)


def portions_of(number_of, total, reach, slope, full):
    weights = [(1 << 20) // math.isqrt(rank ** slope) + 1 for rank in range(1, number_of + 1)]
    largest = reach if full else min(reach, max(-(-total // number_of), total * weights[0] // sum(weights)))
    least = 1 if total - largest >= number_of - 1 else 0
    given, surplus = [largest] + [least] * (number_of - 1), total - largest - least * (number_of - 1)
    while surplus > 0:
        movable = [i for i in range(1, number_of) if given[i] < largest] or [i for i in range(1, number_of) if given[i] < reach]
        whole, budget = sum([weights[i] for i in movable]), surplus
        for i in movable:
            extra = min(reach - given[i], max(1, budget * weights[i] // whole), surplus)
            given[i] = given[i] + extra
            surplus = surplus - extra
    return np.array(given)


def bell_draw(stream_key, extent, deviation, most, pieces=(), kind=jnp.bfloat16):
    drawn = jax.random.normal(stream_key, extent, jnp.float32) * deviation
    if len(pieces) > 0:
        drawn = level_of(stream_key, extent, pieces, -0.22, 0.18) * drawn
    return jnp.clip(drawn, min=-most, max=most).astype(kind)


def setup_inputs(seed: int = 0) -> dict:
    streams_of = jax.random.split(jax.random.key(seed), 8)
    layer_input = bell_draw(streams_of[0], (TOKENS, D), 1.0, 6.0, ((0, 16),))
    out_grad = bell_draw(streams_of[1], (TOKENS, D), 1.0, 6.0, ((0, 16),))
    expert_ids_keys = jax.random.split(jax.random.fold_in(streams_of[2], 1), TOKENS // TOK_DEV)
    expert_ids_turns = jax.random.permutation(jax.random.fold_in(streams_of[2], 3), TOKENS // TOK_DEV)
    expert_ids = jax.vmap(lambda own, number: assign_block(jax.random.fold_in(streams_of[2], 2), own, number, TOK_DEV, EXPERTS, TOP, CAP, 1))(expert_ids_keys, expert_ids_turns).reshape((TOKENS, TOP))
    gate_probs = jnp.clip(0.1 + 0.9 * jax.random.uniform(streams_of[3], (TOKENS, TOP), jnp.float32) ** level_of(streams_of[3], (TOKENS, TOP), ((0, 16),), -0.2, 0.2), 0.1, 1.0)
    gate_proj = bell_draw(streams_of[4], (EXPERTS, D, FF), D ** -0.5, 0.09375, ((0, 16),))
    up_proj = bell_draw(streams_of[5], (EXPERTS, D, FF), D ** -0.5, 0.09375, ((0, 16),))
    down_proj = bell_draw(streams_of[6], (EXPERTS, FF, D), FF ** -0.5, 0.1875, ((0, 16),))
    return {"layer_input": layer_input, "out_grad": out_grad, "expert_ids": expert_ids, "gate_probs": gate_probs, "gate_proj": gate_proj, "up_proj": up_proj, "down_proj": down_proj}


def slot_ranks(flat_ids, experts_count):
    onehot = (flat_ids[:, None] == jnp.arange(experts_count, dtype=jnp.int32)[None, :]).astype(jnp.int32)
    running = jnp.cumsum(onehot, axis=0)
    return jnp.sum((running - 1) * onehot, axis=1).astype(jnp.int32)


def expert_backward(in_rows, grad_rows, gate_mat, up_mat, down_mat):
    gate_pre = jnp.dot(in_rows, gate_mat, preferred_element_type=jnp.float32)
    up_pre = jnp.dot(in_rows, up_mat, preferred_element_type=jnp.float32)
    hidden_grad = lax.dot_general(grad_rows, down_mat, (((1,), (1,)), ((), ())), preferred_element_type=jnp.float32)
    sigmoid = jax.nn.sigmoid(gate_pre)
    gate_grad = (hidden_grad * up_pre * sigmoid * (1.0 + gate_pre * (1.0 - sigmoid))).astype(jnp.bfloat16)
    up_grad = (hidden_grad * gate_pre * sigmoid).astype(jnp.bfloat16)
    back_gate = lax.dot_general(gate_grad, gate_mat, (((1,), (1,)), ((), ())), preferred_element_type=jnp.float32)
    back_up = lax.dot_general(up_grad, up_mat, (((1,), (1,)), ((), ())), preferred_element_type=jnp.float32)
    return back_gate + back_up


def reference(layer_input, out_grad, expert_ids, gate_probs, gate_proj, up_proj, down_proj):
    features = layer_input.shape[1]
    per_dev = TOK_DEV * TOP
    blocks = expert_ids.reshape(N_EP, per_dev).astype(jnp.int32)
    slot_rank = jax.vmap(lambda flat_ids: slot_ranks(flat_ids, EXPERTS))(blocks)
    source = jnp.arange(N_EP, dtype=jnp.int32)[:, None]
    token_index = source * TOK_DEV + jnp.arange(per_dev, dtype=jnp.int32)[None, :] // TOP
    column = (source * CAP + slot_rank).astype(jnp.int32)
    slot_token = jnp.full((EXPERTS, N_EP * CAP), TOKENS, jnp.int32).at[blocks, column].set(token_index.astype(jnp.int32))
    slot_prob = jnp.zeros((EXPERTS, N_EP * CAP), jnp.float32).at[blocks, column].set(gate_probs.reshape(N_EP, per_dev).astype(jnp.float32))
    padded_in = jnp.concatenate([layer_input, jnp.zeros((1, features), layer_input.dtype)], 0)
    padded_grad = jnp.concatenate([out_grad, jnp.zeros((1, features), out_grad.dtype)], 0)

    def per_expert(running_sum, expert_items):
        gate_mat, up_mat, down_mat, tokens_here, probs_here = expert_items
        result = expert_backward(padded_in[tokens_here], padded_grad[tokens_here], gate_mat, up_mat, down_mat).astype(jnp.bfloat16)
        running_sum = running_sum.at[tokens_here].add(result.astype(jnp.float32) * probs_here[:, None])
        return running_sum, None

    start_sum = jnp.zeros((TOKENS + 1, features), jnp.float32)
    running_sum, unused = lax.scan(per_expert, start_sum, (gate_proj, up_proj, down_proj, slot_token, slot_prob))
    return running_sum[:TOKENS].astype(jnp.bfloat16)
```

```python
import functools

import jax
import jax.numpy as jnp
from jax import lax
from jax.experimental import pallas as pl
from jax.experimental.pallas import tpu as pltpu
from jax.sharding import PartitionSpec as P

MESH = pl.DeviceIdType.MESH
NT = (((1,), (1,)), ((), ()))


def kernel(cap, x_hbm, g_hbm, ids_ref, prob_ref, wg_hbm, wu_hbm, wd_hbm, out_ref,
           raw, tabs, stage, comp, part, rc, rr, total, r3, sel, selt, wgv, wuv, wdv, gg, ug, pw, fin,
           send_sem, recv_sem, load_sem):
    me, core = lax.axis_index("ep"), lax.axis_index("dp")
    z, y, x = me // 4, (me // 2) % 2, me % 2
    planes, rows, features = raw.shape[0], raw.shape[2], raw.shape[3]
    hidden, experts = wgv.shape[1], tabs.shape[2] // 2
    cut = features // 2
    f32, bf16 = jnp.float32, jnp.bfloat16
    ad = core == (x + y) % 2
    bc = core != (x + y) % 2
    off1 = jnp.where(ad, 0, cap)
    tab1 = jnp.where(ad, 0, 1)
    inner = (z % (planes - 1)) != 0
    outer = (z % (planes - 1)) == 0
    far = z // 2
    source = [z, z + 1 - 2 * (z % 2), 2 - far, 3 * (1 - far)]
    peer_x, peer_y = z * 4 + y * 2 + (1 - x), z * 4 + (1 - y) * 2 + x
    to_x, to_y, to_core = {"ep": peer_x}, {"ep": peer_y}, {"dp": 1 - core}
    column = [{"ep": s * 4 + y * 2 + x} for s in source]
    above = {"ep": jnp.minimum(z + 1, planes - 1) * 4 + y * 2 + x}
    below = {"ep": jnp.maximum(z - 1, 0) * 4 + y * 2 + x}
    h0, h1 = pl.ds(0, cut), pl.ds(cut, cut)
    lo, hi = pl.ds(0, cap), pl.ds(cap, cap)
    own1 = pl.ds(pl.multiple_of(off1, 16), cap)
    other1 = pl.ds(pl.multiple_of(cap - off1, 16), cap)

    kinds = ("ru", "rd", "tu", "td", "rx", "ry", "tx", "ty", "t2", "sx", "sy", "px", "py", "qx", "qy", "zz", "dp")
    sent, staged = [], {}

    def number(kind, i):
        return kinds.index(kind) * planes + i

    def make(kind, i, src, dst, to, got=None):
        return pltpu.make_async_remote_copy(
            src_ref=src, dst_ref=dst, send_sem=send_sem.at[number(kind, i)],
            recv_sem=recv_sem.at[number(kind, i if got is None else got)],
            device_id=to, device_id_type=MESH,
        )

    def send(cond, kind, i, ends, to, got=None):
        make(kind, i, *ends(), to, got).start()
        done = lambda: make(kind, i, *ends(), to, got).wait_send()
        if kind in ("sx", "sy"):
            staged[kind, i] = done
        else:
            sent.append((cond, done))

    def arrive(kind, i, dst, to):
        make(kind, i, dst, dst, to).wait_recv()

    def when(cond, body):
        pl.when(cond)(body)

    loads = [
        pltpu.make_async_copy(wg_hbm.at[0], wgv, load_sem.at[2]),
        pltpu.make_async_copy(wu_hbm.at[0], wuv, load_sem.at[3]),
        pltpu.make_async_copy(wd_hbm.at[0], wdv, load_sem.at[4]),
    ]

    def own_copies():
        return [
            pltpu.make_async_copy(x_hbm, raw.at[z, 0], load_sem.at[0]),
            pltpu.make_async_copy(g_hbm, raw.at[z, 1], load_sem.at[1]),
        ]

    def begin():
        for copy in own_copies():
            copy.start()

    when(ad, begin)
    for copy in loads:
        copy.start()

    barrier = pltpu.get_barrier_semaphore()
    greeted = [to_x, to_y, to_core]
    greeted += column[1:]
    for other in greeted:
        pl.semaphore_signal(barrier, inc=1, device_id=other, device_id_type=MESH)

    def table():
        name = lax.broadcasted_iota(jnp.int32, (rows, 128), 1)
        count = jnp.zeros((rows, 128), f32)
        prob = jnp.zeros((rows, 128), f32)
        for k in range(ids_ref.shape[1]):
            hit = ids_ref[:, k:k + 1] == name
            count = count + jnp.where(hit, 1.0, 0.0)
            prob = prob + jnp.where(hit, prob_ref[:, k:k + 1], 0.0)
        before = lax.broadcasted_iota(jnp.int32, (rows, rows), 1) < lax.broadcasted_iota(jnp.int32, (rows, rows), 0)
        lower = jnp.where(before, 1.0, 0.0).astype(bf16)
        rank = jnp.dot(lower, count.astype(bf16), preferred_element_type=f32)
        code = jnp.where(count > 0.5, rank, -1.0)
        tabs[z, 0, 0:experts, :] = code.T[0:experts]
        tabs[z, 0, experts:, :] = prob.T[0:experts]

    when(ad, table)
    pl.semaphore_wait(barrier, len(greeted))

    def gather_z(i, cond):
        s = source[i]

        def body():
            if i == 0:
                for copy in own_copies():
                    copy.wait()
            else:
                n = jnp.where(s < z, 0, planes) + s
                arrive("tu", n, tabs.at[s, 0], column[i])
                arrive("ru", n, raw.at[s], column[i])

        when(cond, body)

    def pass_z(i, cond):
        s = source[i]
        go_up = cond & (s <= z) & (z < planes - 1)
        go_down = cond & (s >= z) & (z > 0)

        def up():
            send(go_up, "tu", s, lambda: (tabs.at[s, 0], tabs.at[s, 0]), above)
            send(go_up, "ru", s, lambda: (raw.at[s], raw.at[s]), above)

        def down():
            send(go_down, "td", s, lambda: (tabs.at[s, 0], tabs.at[s, 0]), below)
            send(go_down, "rd", s, lambda: (raw.at[s], raw.at[s]), below)

        when(go_up, up)
        when(go_down, down)

    def spread(i):
        s = source[i]

        def body():
            send(ad, "tx", i, lambda: (tabs.at[s, 0], tabs.at[s, 0]), to_x)
            send(ad, "ty", i, lambda: (tabs.at[s, 0], tabs.at[s, 1]), to_y)
            send(ad, "rx", i, lambda: (raw.at[s, :, :, h0], raw.at[s, :, :, h0]), to_x)
            send(ad, "ry", i, lambda: (raw.at[s, :, :, h1], raw.at[s, :, :, h1]), to_y)

        when(ad, body)

    slot = lax.broadcasted_iota(jnp.int32, (cap, rows), 0).astype(f32)

    def build(i, h, t, target):
        s = source[i]
        for n, e in ((0, target), (1, me)):
            a = jnp.where(slot == tabs[s, t, pl.ds(e, 1), :], 1.0, 0.0)
            sel[i, h, n * cap:(n + 1) * cap, :] = a.astype(bf16)
            selt[i, h, n] = a.T.astype(bf16)

    step = 256

    def pack(i, h, to_rows):
        s = source[i]
        picker = sel[i, h]

        @pl.loop(0, cut // step)
        def _(n):
            local = pl.ds(pl.multiple_of(n * step, step), step)
            cols = pl.ds(pl.multiple_of(h * cut + n * step, step), step)
            for k in range(2):
                picked = jnp.dot(picker, raw[s, k, :, cols], preferred_element_type=f32).astype(bf16)
                stage[i % 2, h, k, :, local] = picked[0:cap]
                comp[i, k, to_rows, cols] = picked[cap:]

    def settle(i):
        for h, kind in ((0, "sy"), (1, "sx")):
            staged.pop((kind, i))()

    def share(i):
        s = source[i]
        if i >= 2:
            settle(i - 2)

        def first():
            arrive("tx", i, tabs.at[s, 0], to_x)
            send(bc, "t2", i, lambda: (tabs.at[s, 0], tabs.at[s, 1]), to_y)
            arrive("rx", i, raw.at[s, :, :, h0], to_x)

        when(bc, first)
        build(i, 0, 0, peer_y)
        pack(i, 0, lo)
        send(None, "sy", i, lambda: (stage.at[i % 2, 0], comp.at[i, :, hi, h0]), to_y)

        def second():
            arrive("ty", i, tabs.at[s, 1], to_y)
            arrive("ry", i, raw.at[s, :, :, h1], to_y)

        when(bc, second)
        build(i, 1, tab1, peer_x)
        pack(i, 1, own1)
        send(None, "sx", i, lambda: (stage.at[i % 2, 1], comp.at[i, :, own1, h1]), to_x)

    def compute(i):
        s = source[i]
        arrive("sy", i, comp.at[i, :, hi, h0], to_y)
        arrive("sx", i, comp.at[i, :, other1, h1], to_x)
        when(ad, lambda: arrive("t2", i, tabs.at[s, 1], to_y))
        for k in range(2):
            hit = slot == tabs[s, k, pl.ds(me, 1), :]
            pw[k * cap:(k + 1) * cap, :] = jnp.sum(
                jnp.where(hit, tabs[s, k, pl.ds(experts + me, 1), :], 0.0), axis=1, keepdims=True)
        tile = 256

        @pl.loop(0, hidden // tile)
        def _(f):
            cols = pl.ds(pl.multiple_of(f * tile, tile), tile)
            gate = jnp.dot(comp[i, 0], wgv[:, cols], preferred_element_type=f32)
            up = jnp.dot(comp[i, 0], wuv[:, cols], preferred_element_type=f32)
            grad = lax.dot_general(comp[i, 1], wdv[cols, :], NT, preferred_element_type=f32)
            s = jax.nn.sigmoid(gate)
            gg[:, cols] = (grad * up * s * (1.0 + gate * (1.0 - s))).astype(bf16)
            ug[:, cols] = (grad * gate * s).astype(bf16)

        wide = 512

        @pl.loop(0, features // wide)
        def _(d):
            cols = pl.ds(pl.multiple_of(d * wide, wide), wide)
            back = lax.dot_general(gg[...], wgv[cols, :], NT, preferred_element_type=f32)
            back = back + lax.dot_general(ug[...], wuv[cols, :], NT, preferred_element_type=f32)
            part[i, :, cols] = (back * pw[...]).astype(bf16)

    def back1(i):
        send(None, "py", i, lambda: (part.at[i, hi, h0], rc.at[i, :, h0]), to_y)
        send(None, "px", i, lambda: (part.at[i, other1, h1], rc.at[i, :, h1]), to_x)

    def merged(i, h, n, mine):
        cols = pl.ds(pl.multiple_of(h * cut + n * step, step), step)
        value = jnp.dot(selt[i, h, 1], part[i, mine, cols], preferred_element_type=f32)
        return cols, value + jnp.dot(selt[i, h, 0], rc[i, :, cols], preferred_element_type=f32)

    def back2(i):
        def body():
            for h, kind, to, out, there, mine in (
                (0, "py", to_y, "qx", to_x, lo), (1, "px", to_x, "qy", to_y, hi)):
                half = (h0, h1)[h]
                arrive(kind, i, rc.at[i, :, half], to)

                @pl.loop(0, cut // step)
                def _(n):
                    cols, value = merged(i, h, n, mine)
                    total[i, :, cols] = value.astype(bf16)

                send(bc, out, i, lambda half=half: (total.at[i, :, half], rr.at[i, :, half]), there)

        when(bc, body)

    def back3(i):
        s = source[i]

        def body():
            if i == 0:
                for j in range(1, planes):
                    arrive("zz", source[j], r3.at[source[j]], column[j])
            for h, kind, to, out, there in ((0, "py", to_y, "qx", to_x), (1, "px", to_x, "qy", to_y)):
                half = (h0, h1)[h]
                arrive(kind, i, rc.at[i, :, half], to)
                arrive(out, i, rr.at[i, :, half], there)

                @pl.loop(0, cut // step)
                def _(n):
                    cols, value = merged(i, h, n, lo)
                    value = value + rr[i, :, cols].astype(f32)
                    if i == 0:
                        for j in range(1, planes):
                            value = value + r3[source[j], :, cols].astype(f32)
                        fin[h, :, pl.ds(pl.multiple_of(n * step, step), step)] = value.astype(bf16)
                    else:
                        total[i, :, cols] = value.astype(bf16)

            if i > 0:
                send(ad, "zz", s, lambda: (total.at[i], r3.at[z]), column[i], got=z)

        when(ad, body)

    gather_z(0, ad)
    spread(0)
    pass_z(0, ad)
    share(0)
    gather_z(1, ad)
    pass_z(1, ad)
    spread(1)
    gather_z(2, ad & inner)
    pass_z(2, ad & inner)
    share(1)
    for copy in loads:
        copy.wait()
    compute(0)
    gather_z(2, ad & outer)
    spread(2)
    gather_z(3, ad & inner)
    pass_z(3, ad & inner)
    share(2)
    compute(1)
    back1(1)
    gather_z(3, ad & outer)
    spread(3)
    back2(1)
    share(3)
    back1(0)
    compute(2)
    back1(2)
    back3(1)
    back2(2)
    compute(3)
    back1(3)
    back3(2)
    back2(3)
    back2(0)
    back3(3)
    back3(0)

    def finish():
        send(ad, "dp", 0, lambda: (fin.at[1 - core], out_ref), to_core)
        out_ref[...] = fin[core]

    when(ad, finish)
    when(bc, lambda: arrive("dp", 0, out_ref, to_core))
    for wait in staged.values():
        wait()
    for cond, wait in sent:
        if cond is None:
            wait()
        else:
            when(cond, wait)


def fused(layer_input, out_grad, expert_ids, gate_probs, gate_proj, up_proj, down_proj):
    experts, halves = lax.axis_size("ep"), lax.axis_size("dp")
    rows, features = layer_input.shape
    hidden = gate_proj.shape[2]
    planes = experts // 4
    cap = capacity(experts, expert_ids.shape)
    cut, bf16, f32 = features // 2, jnp.bfloat16, jnp.float32
    vmem, hbm = pl.BlockSpec(memory_space=pltpu.VMEM), pl.BlockSpec(memory_space=pl.ANY)
    count = 17 * planes
    return pl.pallas_call(
        functools.partial(kernel, cap),
        name="fused_backward",
        out_shape=jax.ShapeDtypeStruct((rows, cut), bf16),
        in_specs=[hbm, hbm, vmem, vmem, hbm, hbm, hbm],
        out_specs=vmem,
        scratch_shapes=[
            pltpu.VMEM((planes, 2, rows, features), bf16),
            pltpu.VMEM((planes, 2, 2 * experts, rows), f32),
            pltpu.VMEM((2, 2, 2, cap, cut), bf16),
            pltpu.VMEM((planes, 2, 2 * cap, features), bf16),
            pltpu.VMEM((planes, 2 * cap, features), bf16),
            pltpu.VMEM((planes, cap, features), bf16),
            pltpu.VMEM((planes, rows, features), bf16),
            pltpu.VMEM((planes, rows, features), bf16),
            pltpu.VMEM((planes, rows, features), bf16),
            pltpu.VMEM((planes, 2, 2 * cap, rows), bf16),
            pltpu.VMEM((planes, 2, 2, rows, cap), bf16),
            pltpu.VMEM((features, hidden), bf16),
            pltpu.VMEM((features, hidden), bf16),
            pltpu.VMEM((hidden, features), bf16),
            pltpu.VMEM((2 * cap, hidden), bf16),
            pltpu.VMEM((2 * cap, hidden), bf16),
            pltpu.VMEM((2 * cap, 1), f32),
            pltpu.VMEM((halves, rows, cut), bf16),
            pltpu.SemaphoreType.DMA((count,)),
            pltpu.SemaphoreType.DMA((count,)),
            pltpu.SemaphoreType.DMA((5,)),
        ],
        compiler_params=pltpu.CompilerParams(
            collective_id=0, has_side_effects=True, vmem_limit_bytes=67043328
        ),
    )(layer_input, out_grad, expert_ids, gate_probs, gate_proj, up_proj, down_proj)


def capacity(experts, shape):
    return 5 * shape[0] * shape[1] // (4 * experts)


def dense(layer_input, out_grad, expert_ids, gate_probs, gate_proj, up_proj, down_proj):
    experts = lax.axis_size("ep")
    halves = lax.axis_size("dp")
    tok_rows, features = layer_input.shape
    half = tok_rows // halves
    core = lax.axis_index("dp")
    start = core * half
    mine_in = lax.dynamic_slice_in_dim(layer_input, start, half, 0)
    mine_grad = lax.dynamic_slice_in_dim(out_grad, start, half, 0)
    ids = lax.dynamic_slice_in_dim(expert_ids, start, half, 0)
    probs = lax.dynamic_slice_in_dim(gate_probs, start, half, 0)
    names = jnp.arange(experts, dtype=jnp.int32)
    table = jnp.sum(
        jnp.where(ids[None, :, :] == names[:, None, None], probs[None, :, :], 0.0), axis=2
    )
    weight = lax.all_to_all(table, "ep", split_axis=0, concat_axis=0, tiled=True).reshape(-1)
    in_rows = lax.all_gather(mine_in, "ep", axis=0, tiled=True)
    grad_rows = lax.all_gather(mine_grad, "ep", axis=0, tiled=True)
    gate_mat, up_mat, down_mat = (gate_proj[0], up_proj[0], down_proj[0])
    nt = (((1,), (1,)), ((), ()))
    gate_pre = jnp.dot(in_rows, gate_mat, preferred_element_type=jnp.float32)
    up_pre = jnp.dot(in_rows, up_mat, preferred_element_type=jnp.float32)
    hidden_grad = lax.dot_general(grad_rows, down_mat, nt, preferred_element_type=jnp.float32)
    s = jax.nn.sigmoid(gate_pre)
    gate_grad = (hidden_grad * up_pre * s * (1.0 + gate_pre * (1.0 - s))).astype(jnp.bfloat16)
    up_grad = (hidden_grad * gate_pre * s).astype(jnp.bfloat16)
    back = lax.dot_general(gate_grad, gate_mat, nt, preferred_element_type=jnp.float32)
    back = back + lax.dot_general(up_grad, up_mat, nt, preferred_element_type=jnp.float32)
    back = (back * weight[:, None]).astype(jnp.bfloat16)
    mine = lax.psum_scatter(back, "ep", scatter_dimension=0, tiled=True)
    return lax.all_to_all(mine, "dp", split_axis=1, concat_axis=0, tiled=True)


def body(*args):
    experts, halves = lax.axis_size("ep"), lax.axis_size("dp")
    rows, features = args[0].shape
    hidden = args[4].shape[2]
    cap = capacity(experts, args[2].shape)
    planes = experts // 4
    held = 2 * features * (planes * (5 * rows + 7 * cap) + 3 * hidden + rows + 8 * cap)
    fits = held < 64 * 10**6 and halves == 2 and experts == 16 and cap % 16 == 0
    return (fused if fits else dense)(*args)


def solution(mesh):
    row = P("ep", None)
    mat = P("ep", None, None)
    return jax.shard_map(
        body, mesh=mesh, in_specs=(row, row, row, row, mat, mat, mat), out_specs=P("ep", "dp"), check_vma=False
    )
```

```python
import functools

import jax
import jax.numpy as jnp
from jax import lax
from jax.experimental import pallas as pl
from jax.experimental.pallas import tpu as pltpu
from jax.sharding import PartitionSpec as P

MESH = pl.DeviceIdType.MESH
NT = (((1,), (1,)), ((), ()))


STEPS = (
    ("gz", 0), ("sp", 0), ("sy", 0), ("sx", 0), ("gz", 1), ("sp", 1), ("go", 2), ("gi", 2),
    ("sp", 2), ("sy", 1), ("sx", 1), ("sx", 2), ("sy", 2), ("go", 3), ("gi", 3), ("cf", 1),
    ("sp", 3), ("cf", 2), ("sx", 3), ("cb", 2), ("sy", 3), ("ca", 2), ("cb", 1), ("cf", 0),
    ("1x", 2), ("2x", 2), ("ca", 1), ("1x", 1), ("2x", 1), ("1y", 2), ("2y", 2), ("1y", 1),
    ("cf", 3), ("cb", 3), ("2y", 1), ("3x", 2), ("ca", 3), ("1x", 3), ("cb", 0), ("3y", 2),
    ("3x", 1), ("2x", 3), ("1y", 3), ("ca", 0), ("3y", 1), ("3x", 3), ("2y", 3), ("1x", 0),
    ("3y", 3), ("1y", 0), ("2x", 0), ("2y", 0), ("3x", 0), ("3y", 0),
)


def kernel(cap, x_hbm, g_hbm, ids_hbm, prob_hbm, wg_hbm, wu_hbm, wd_hbm, out_ref,
           raw, tabs, stage, comp, part, rc, rr, total, r3, sel, selt, wgv, wuv, wdv, gg, ug, pw, fin, ids_ref, prob_ref,
           send_sem, recv_sem, load_sem):
    me, core = lax.axis_index("ep"), lax.axis_index("dp")
    z, y, x = me // 4, (me // 2) % 2, me % 2
    planes, rows, features = raw.shape[0], raw.shape[2], raw.shape[3]
    hidden, experts = wgv.shape[1], tabs.shape[2] // 2
    cut = features // 2
    f32, bf16 = jnp.float32, jnp.bfloat16
    ad = core == (x + y) % 2
    bc = core != (x + y) % 2
    off1 = jnp.where(ad, 0, cap)
    tab1 = jnp.where(ad, 0, 1)
    inner = (z % (planes - 1)) != 0
    outer = (z % (planes - 1)) == 0
    far = z // 2
    source = [z, z + 1 - 2 * (z % 2), 2 - far, 3 * (1 - far)]
    peer_x, peer_y = z * 4 + y * 2 + (1 - x), z * 4 + (1 - y) * 2 + x
    to_x, to_y, to_core = {"ep": peer_x}, {"ep": peer_y}, {"dp": 1 - core}
    column = [{"ep": s * 4 + y * 2 + x} for s in source]
    above = {"ep": jnp.minimum(z + 1, planes - 1) * 4 + y * 2 + x}
    below = {"ep": jnp.maximum(z - 1, 0) * 4 + y * 2 + x}
    h0, h1 = pl.ds(0, cut), pl.ds(cut, cut)
    lo, hi = pl.ds(0, cap), pl.ds(cap, cap)
    own1 = pl.ds(pl.multiple_of(off1, 16), cap)
    other1 = pl.ds(pl.multiple_of(cap - off1, 16), cap)

    kinds = ("ru", "rd", "tu", "td", "rx", "ry", "tx", "ty", "t2", "sx", "sy", "px", "py", "qx", "qy", "z0", "z1", "dp")
    sent, staged = [], {}

    def number(kind, i):
        return kinds.index(kind) * planes + i

    def make(kind, i, src, dst, to, got=None):
        return pltpu.make_async_remote_copy(
            src_ref=src, dst_ref=dst, send_sem=send_sem.at[number(kind, i)],
            recv_sem=recv_sem.at[number(kind, i if got is None else got)],
            device_id=to, device_id_type=MESH,
        )

    def send(cond, kind, i, ends, to, got=None):
        make(kind, i, *ends(), to, got).start()
        done = lambda: make(kind, i, *ends(), to, got).wait_send()
        if kind in ("sx", "sy"):
            staged[kind, i] = done
        else:
            sent.append((cond, done))

    def arrive(kind, i, dst, to):
        make(kind, i, dst, dst, to).wait_recv()

    def when(cond, body):
        pl.when(cond)(body)

    loads = [
        pltpu.make_async_copy(wg_hbm.at[0], wgv, load_sem.at[2]),
        pltpu.make_async_copy(wu_hbm.at[0], wuv, load_sem.at[3]),
        pltpu.make_async_copy(wd_hbm.at[0], wdv, load_sem.at[4]),
    ]

    def own_lists():
        return [
            pltpu.make_async_copy(ids_hbm, ids_ref, load_sem.at[5]),
            pltpu.make_async_copy(prob_hbm, prob_ref, load_sem.at[6]),
        ]

    def own_copies():
        return [
            pltpu.make_async_copy(x_hbm, raw.at[z, 0], load_sem.at[0]),
            pltpu.make_async_copy(g_hbm, raw.at[z, 1], load_sem.at[1]),
        ]

    def begin():
        for copy in own_lists() + own_copies():
            copy.start()

    when(ad, begin)
    for copy in loads:
        copy.start()

    barrier = pltpu.get_barrier_semaphore()
    greeted = [to_x, to_y, to_core]
    greeted += column[1:]
    for other in greeted:
        pl.semaphore_signal(barrier, inc=1, device_id=other, device_id_type=MESH)

    def table():
        for copy in own_lists():
            copy.wait()
        name = lax.broadcasted_iota(jnp.int32, (rows, 128), 1)
        count = jnp.zeros((rows, 128), f32)
        prob = jnp.zeros((rows, 128), f32)
        for k in range(ids_ref.shape[1]):
            hit = ids_ref[:, k:k + 1] == name
            count = count + jnp.where(hit, 1.0, 0.0)
            prob = prob + jnp.where(hit, prob_ref[:, k:k + 1], 0.0)
        before = lax.broadcasted_iota(jnp.int32, (rows, rows), 1) < lax.broadcasted_iota(jnp.int32, (rows, rows), 0)
        lower = jnp.where(before, 1.0, 0.0).astype(bf16)
        rank = jnp.dot(lower, count.astype(bf16), preferred_element_type=f32)
        code = jnp.where(count > 0.5, rank, -1.0)
        tabs[z, 0, 0:experts, :] = code.T[0:experts]
        tabs[z, 0, experts:, :] = prob.T[0:experts]

    when(ad, table)
    pl.semaphore_wait(barrier, len(greeted))

    def gather_z(i, cond):
        s = source[i]

        def body():
            if i == 0:
                for copy in own_copies():
                    copy.wait()
            else:
                n = jnp.where(s < z, 0, planes) + s
                arrive("tu", n, tabs.at[s, 0], column[i])
                arrive("ru", n, raw.at[s], column[i])

        when(cond, body)

    def pass_z(i, cond):
        s = source[i]
        go_up = cond & (s <= z) & (z < planes - 1)
        go_down = cond & (s >= z) & (z > 0)

        def up():
            send(go_up, "tu", s, lambda: (tabs.at[s, 0], tabs.at[s, 0]), above)
            send(go_up, "ru", s, lambda: (raw.at[s], raw.at[s]), above)

        def down():
            send(go_down, "td", s, lambda: (tabs.at[s, 0], tabs.at[s, 0]), below)
            send(go_down, "rd", s, lambda: (raw.at[s], raw.at[s]), below)

        when(go_up, up)
        when(go_down, down)

    def spread(i):
        s = source[i]

        def body():
            send(ad, "tx", i, lambda: (tabs.at[s, 0], tabs.at[s, 0]), to_x)
            send(ad, "ty", i, lambda: (tabs.at[s, 0], tabs.at[s, 1]), to_y)
            send(ad, "rx", i, lambda: (raw.at[s, :, :, h0], raw.at[s, :, :, h0]), to_x)
            send(ad, "ry", i, lambda: (raw.at[s, :, :, h1], raw.at[s, :, :, h1]), to_y)

        when(ad, body)

    slot = lax.broadcasted_iota(jnp.int32, (cap, rows), 0).astype(f32)

    def build(i, h, t, target):
        s = source[i]
        for n, e in ((0, target), (1, me)):
            a = jnp.where(slot == tabs[s, t, pl.ds(e, 1), :], 1.0, 0.0)
            sel[i, h, n * cap:(n + 1) * cap, :] = a.astype(bf16)
            selt[i, h, n] = a.T.astype(bf16)

    step = cut // 2 if cut % 256 == 0 else cut

    def pack(i, h, to_rows):
        s = source[i]
        picker = sel[i, h]

        @pl.loop(0, cut // step)
        def _(n):
            local = pl.ds(pl.multiple_of(n * step, 128), step)
            cols = pl.ds(pl.multiple_of(h * cut + n * step, 128), step)
            for k in range(2):
                picked = jnp.dot(picker, raw[s, k, :, cols], preferred_element_type=f32).astype(bf16)
                stage[i % 2, h, k, :, local] = picked[0:cap]
                comp[i, k, to_rows, cols] = picked[cap:]

    def share_y(i):
        s = source[i]
        if i >= 2:
            staged.pop(("sy", i - 2))()

        def first():
            arrive("tx", i, tabs.at[s, 0], to_x)
            send(bc, "t2", i, lambda: (tabs.at[s, 0], tabs.at[s, 1]), to_y)
            arrive("rx", i, raw.at[s, :, :, h0], to_x)

        when(bc, first)
        build(i, 0, 0, peer_y)
        pack(i, 0, lo)
        send(None, "sy", i, lambda: (stage.at[i % 2, 0], comp.at[i, :, hi, h0]), to_y)

    def share_x(i):
        s = source[i]
        if i >= 2:
            staged.pop(("sx", i - 2))()

        def second():
            arrive("ty", i, tabs.at[s, 1], to_y)
            arrive("ry", i, raw.at[s, :, :, h1], to_y)

        when(bc, second)
        build(i, 1, tab1, peer_x)
        pack(i, 1, own1)
        send(None, "sx", i, lambda: (stage.at[i % 2, 1], comp.at[i, :, own1, h1]), to_x)

    def forward(i):
        s = source[i]
        arrive("sy", i, comp.at[i, :, hi, h0], to_y)
        arrive("sx", i, comp.at[i, :, other1, h1], to_x)
        when(ad, lambda: arrive("t2", i, tabs.at[s, 1], to_y))
        for k in range(2):
            hit = slot == tabs[s, k, pl.ds(me, 1), :]
            pw[i, k * cap:(k + 1) * cap, :] = jnp.sum(
                jnp.where(hit, tabs[s, k, pl.ds(experts + me, 1), :], 0.0), axis=1, keepdims=True)
        tile = 256

        @pl.loop(0, hidden // tile)
        def _(f):
            cols = pl.ds(pl.multiple_of(f * tile, tile), tile)
            gate = jnp.dot(comp[i, 0], wgv[:, cols], preferred_element_type=f32)
            up = jnp.dot(comp[i, 0], wuv[:, cols], preferred_element_type=f32)
            grad = lax.dot_general(comp[i, 1], wdv[cols, :], NT, preferred_element_type=f32)
            s = jax.nn.sigmoid(gate)
            gg[i, :, cols] = (grad * up * s * (1.0 + gate * (1.0 - s))).astype(bf16)
            ug[i, :, cols] = (grad * gate * s).astype(bf16)

    def backward(i, h):
        @pl.loop(0, cut // step)
        def _(d):
            cols = pl.ds(pl.multiple_of(h * cut + d * step, 128), step)
            back = lax.dot_general(gg[i], wgv[cols, :], NT, preferred_element_type=f32)
            back = back + lax.dot_general(ug[i], wuv[cols, :], NT, preferred_element_type=f32)
            part[i, :, cols] = (back * pw[i]).astype(bf16)

    def back1_y(i):
        send(None, "py", i, lambda: (part.at[i, hi, h0], rc.at[i, :, h0]), to_y)

    def back1_x(i):
        send(None, "px", i, lambda: (part.at[i, other1, h1], rc.at[i, :, h1]), to_x)

    def merged(i, h, n, mine):
        cols = pl.ds(pl.multiple_of(h * cut + n * step, 128), step)
        value = jnp.dot(selt[i, h, 1], part[i, mine, cols], preferred_element_type=f32)
        return cols, value + jnp.dot(selt[i, h, 0], rc[i, :, cols], preferred_element_type=f32)

    routes = (("py", to_y, "qx", to_x, h0, lo), ("px", to_x, "qy", to_y, h1, hi))

    def back2(i, h):
        kind, to, out, there, half, mine = routes[h]

        def body():
            arrive(kind, i, rc.at[i, :, half], to)

            @pl.loop(0, cut // step)
            def _(n):
                cols, value = merged(i, h, n, mine)
                total[i, :, cols] = value.astype(bf16)

            send(bc, out, i, lambda: (total.at[i, :, half], rr.at[i, :, half]), there)

        when(bc, body)

    def back3(i, h):
        s = source[i]
        kind, to, out, there, half, mine = routes[h]
        home = ("z0", "z1")[h]

        def body():
            arrive(kind, i, rc.at[i, :, half], to)
            arrive(out, i, rr.at[i, :, half], there)
            if i == 0:
                for j in range(1, planes):
                    arrive(home, source[j], r3.at[source[j], :, half], column[j])

            @pl.loop(0, cut // step)
            def _(n):
                cols, value = merged(i, h, n, lo)
                value = value + rr[i, :, cols].astype(f32)
                if i == 0:
                    for j in range(1, planes):
                        value = value + r3[source[j], :, cols].astype(f32)
                    fin[h, :, pl.ds(pl.multiple_of(n * step, 128), step)] = value.astype(bf16)
                else:
                    total[i, :, cols] = value.astype(bf16)

            if i > 0:
                send(ad, home, s, lambda: (total.at[i, :, half], r3.at[z, :, half]), column[i], got=z)

        when(ad, body)
        if i == 0:
            over = ad & (core != h)
            when(over, lambda: send(over, "dp", h, lambda: (fin.at[h], out_ref), to_core))

    ops = {
        "sp": spread,
        "gz": lambda i: (gather_z(i, ad), pass_z(i, ad)),
        "gi": lambda i: (gather_z(i, ad & inner), pass_z(i, ad & inner)),
        "go": lambda i: gather_z(i, ad & outer),
        "sy": share_y, "sx": share_x, "cf": forward,
        "ca": lambda i: backward(i, 0), "cb": lambda i: backward(i, 1),
        "1y": back1_y, "1x": back1_x,
        "2y": lambda i: back2(i, 0), "2x": lambda i: back2(i, 1),
        "3y": lambda i: back3(i, 0), "3x": lambda i: back3(i, 1),
    }
    for name, i in STEPS:
        if name == "cf":
            while loads:
                loads.pop().wait()
        ops[name](i)

    def finish():
        out_ref[...] = fin[core]

    when(ad, finish)
    when(bc, lambda: arrive("dp", core, out_ref, to_core))
    for wait in staged.values():
        wait()
    for cond, wait in sent:
        if cond is None:
            wait()
        else:
            when(cond, wait)


def fused(layer_input, out_grad, expert_ids, gate_probs, gate_proj, up_proj, down_proj):
    experts, halves = lax.axis_size("ep"), lax.axis_size("dp")
    rows, features = layer_input.shape
    hidden = gate_proj.shape[2]
    planes = experts // 4
    cap = capacity(experts, expert_ids.shape)
    cut, bf16, f32 = features // 2, jnp.bfloat16, jnp.float32
    vmem, hbm = pl.BlockSpec(memory_space=pltpu.VMEM), pl.BlockSpec(memory_space=pl.ANY)
    count = 18 * planes
    return pl.pallas_call(
        functools.partial(kernel, cap),
        name="fused_backward",
        out_shape=jax.ShapeDtypeStruct((rows, cut), bf16),
        in_specs=[hbm] * 7,
        out_specs=vmem,
        scratch_shapes=[
            pltpu.VMEM((planes, 2, rows, features), bf16),
            pltpu.VMEM((planes, 2, 2 * experts, rows), f32),
            pltpu.VMEM((2, 2, 2, cap, cut), bf16),
            pltpu.VMEM((planes, 2, 2 * cap, features), bf16),
            pltpu.VMEM((planes, 2 * cap, features), bf16),
            pltpu.VMEM((planes, cap, features), bf16),
            pltpu.VMEM((planes, rows, features), bf16),
            pltpu.VMEM((planes, rows, features), bf16),
            pltpu.VMEM((planes, rows, features), bf16),
            pltpu.VMEM((planes, 2, 2 * cap, rows), bf16),
            pltpu.VMEM((planes, 2, 2, rows, cap), bf16),
            pltpu.VMEM((features, hidden), bf16),
            pltpu.VMEM((features, hidden), bf16),
            pltpu.VMEM((hidden, features), bf16),
            pltpu.VMEM((planes, 2 * cap, hidden), bf16),
            pltpu.VMEM((planes, 2 * cap, hidden), bf16),
            pltpu.VMEM((planes, 2 * cap, 1), f32),
            pltpu.VMEM((halves, rows, cut), bf16),
            pltpu.VMEM(expert_ids.shape, jnp.int32),
            pltpu.VMEM(gate_probs.shape, f32),
            pltpu.SemaphoreType.DMA((count,)),
            pltpu.SemaphoreType.DMA((count,)),
            pltpu.SemaphoreType.DMA((7,)),
        ],
        compiler_params=pltpu.CompilerParams(
            collective_id=0, has_side_effects=True, vmem_limit_bytes=67043328
        ),
    )(layer_input, out_grad, expert_ids, gate_probs, gate_proj, up_proj, down_proj)


def capacity(experts, shape):
    return 5 * shape[0] * shape[1] // (4 * experts)


def dense(layer_input, out_grad, expert_ids, gate_probs, gate_proj, up_proj, down_proj):
    experts = lax.axis_size("ep")
    halves = lax.axis_size("dp")
    tok_rows, features = layer_input.shape
    half = tok_rows // halves
    core = lax.axis_index("dp")
    start = core * half
    mine_in = lax.dynamic_slice_in_dim(layer_input, start, half, 0)
    mine_grad = lax.dynamic_slice_in_dim(out_grad, start, half, 0)
    ids = lax.dynamic_slice_in_dim(expert_ids, start, half, 0)
    probs = lax.dynamic_slice_in_dim(gate_probs, start, half, 0)
    names = jnp.arange(experts, dtype=jnp.int32)
    table = jnp.sum(
        jnp.where(ids[None, :, :] == names[:, None, None], probs[None, :, :], 0.0), axis=2
    )
    weight = lax.all_to_all(table, "ep", split_axis=0, concat_axis=0, tiled=True).reshape(-1)
    in_rows = lax.all_gather(mine_in, "ep", axis=0, tiled=True)
    grad_rows = lax.all_gather(mine_grad, "ep", axis=0, tiled=True)
    gate_mat, up_mat, down_mat = (gate_proj[0], up_proj[0], down_proj[0])
    nt = (((1,), (1,)), ((), ()))
    gate_pre = jnp.dot(in_rows, gate_mat, preferred_element_type=jnp.float32)
    up_pre = jnp.dot(in_rows, up_mat, preferred_element_type=jnp.float32)
    hidden_grad = lax.dot_general(grad_rows, down_mat, nt, preferred_element_type=jnp.float32)
    s = jax.nn.sigmoid(gate_pre)
    gate_grad = (hidden_grad * up_pre * s * (1.0 + gate_pre * (1.0 - s))).astype(jnp.bfloat16)
    up_grad = (hidden_grad * gate_pre * s).astype(jnp.bfloat16)
    back = lax.dot_general(gate_grad, gate_mat, nt, preferred_element_type=jnp.float32)
    back = back + lax.dot_general(up_grad, up_mat, nt, preferred_element_type=jnp.float32)
    back = (back * weight[:, None]).astype(jnp.bfloat16)
    mine = lax.psum_scatter(back, "ep", scatter_dimension=0, tiled=True)
    return lax.all_to_all(mine, "dp", split_axis=1, concat_axis=0, tiled=True)


def body(*args):
    experts, halves = lax.axis_size("ep"), lax.axis_size("dp")
    rows, features = args[0].shape
    hidden = args[4].shape[2]
    cap = capacity(experts, args[2].shape)
    planes = experts // 4
    held = 2 * features * (planes * (5 * rows + 7 * cap) + 3 * hidden + rows + 8 * cap)
    fits = held < 64 * 10**6 and halves == 2 and experts == 16 and cap % 16 == 0
    return (fused if fits else dense)(*args)


def solution(mesh):
    row = P("ep", None)
    mat = P("ep", None, None)
    return jax.shard_map(
        body, mesh=mesh, in_specs=(row, row, row, row, mat, mat, mat), out_specs=P("ep", "dp"), check_vma=False
    )
```

```python
import functools

import jax
import jax.numpy as jnp
from jax import lax
from jax.experimental import pallas as pl
from jax.experimental.pallas import tpu as pltpu
from jax.sharding import PartitionSpec as P

MESH = pl.DeviceIdType.MESH
NT = (((1,), (1,)), ((), ()))


LINE = 4

STEPS = (
    ("gz", 0), ("sp", 0), ("v0", 0), ("tb", 0), ("v1", 0), ("sx", 0), ("sy", 0), ("gz", 1), ("gi", 2),
    ("sp", 1), ("sx", 1), ("za", 0), ("sy", 1), ("zb", 0), ("cf", 0), ("go", 2), ("cb", 0),
    ("sp", 2), ("gi", 3), ("ra", 1), ("rb", 1), ("sx", 2), ("sy", 2), ("cf", 1), ("ca", 1),
    ("cb", 1), ("go", 3), ("sp", 3), ("ra", 2), ("rb", 2), ("sy", 3), ("sx", 3), ("cf", 2),
    ("1x", 1), ("ca", 2), ("1y", 2), ("1y", 1), ("cb", 2), ("2y", 2), ("1x", 2), ("ca", 0),
    ("2x", 2), ("rb", 3), ("2x", 1), ("2y", 1), ("ra", 3), ("cf", 3), ("3y", 2), ("cb", 3),
    ("ca", 3), ("3x", 2), ("1x", 3), ("2x", 3), ("1y", 3), ("2y", 3), ("1x", 0), ("2x", 0),
    ("3x", 1), ("1y", 0), ("3y", 1), ("2y", 0), ("3x", 3), ("3y", 3), ("3x", 0), ("3y", 0),
)


def kernel(cap, x_hbm, g_hbm, ids_hbm, prob_hbm, wg_hbm, wu_hbm, wd_hbm, out_ref,
           raw, rawv, tabs, stage, stagev, comp, part, rc, rr, r3, sel, selt, wgv, wuv, wdv, gg, ug, pw, ids_ref, prob_ref,
           send_sem, recv_sem, load_sem):
    me, core = lax.axis_index("ep"), lax.axis_index("dp")
    z, y, x = me // 4, (me // 2) % 2, me % 2
    planes, rows, features = comp.shape[0], raw.shape[2], comp.shape[3]
    hidden, experts = wgv.shape[1], tabs.shape[2] // 2
    cut = features // 2
    f32, bf16 = jnp.float32, jnp.bfloat16
    ad = core == (x + y) % 2
    bc = core != (x + y) % 2
    off1 = jnp.where(ad, 0, cap)
    tab1 = jnp.where(ad, 0, 1)
    inner = (z % (planes - 1)) != 0
    outer = (z % (planes - 1)) == 0
    far = z // 2
    source = [z, z + 1 - 2 * (z % 2), 2 - far, 3 * (1 - far)]
    peer_x, peer_y = z * 4 + y * 2 + (1 - x), z * 4 + (1 - y) * 2 + x
    to_x, to_y, to_core = {"ep": peer_x}, {"ep": peer_y}, {"dp": 1 - core}
    column = [{"ep": s * 4 + y * 2 + x} for s in source]
    above = {"ep": jnp.minimum(z + 1, planes - 1) * 4 + y * 2 + x}
    below = {"ep": jnp.maximum(z - 1, 0) * 4 + y * 2 + x}
    near, aside = raw.shape[3] // 2, rawv.shape[4]
    a0, a1, av = pl.ds(0, near), pl.ds(near, near), pl.ds(2 * near, aside)
    h0, h1 = pl.ds(0, cut), pl.ds(cut, cut)
    slots = (pl.ds(0, cap), pl.ds(cap, cap))
    end = (planes - 1) * far * 4 + y * 2 + x
    toward = {"ep": jnp.where(inner, 2 - far, 1 + far) * 4 + y * 2 + x}
    to_end = {"ep": end}
    lo, hi = pl.ds(0, cap), pl.ds(cap, cap)
    own1 = pl.ds(pl.multiple_of(off1, 16), cap)
    other1 = pl.ds(pl.multiple_of(cap - off1, 16), cap)

    kinds = ("ru", "rd", "tu", "td", "rx", "ry", "tx", "ty", "t2", "sx", "sy", "px", "py", "qx", "qy", "z0", "z1", "dp",
             "va", "vb", "ea", "eb", "vx", "vy", "wx", "wy")
    sent, staged = [], {}

    def number(kind, i):
        return kinds.index(kind) * planes + i

    def make(kind, i, src, dst, to, got=None):
        return pltpu.make_async_remote_copy(
            src_ref=src, dst_ref=dst, send_sem=send_sem.at[number(kind, i)],
            recv_sem=recv_sem.at[number(kind, i if got is None else got)],
            device_id=to, device_id_type=MESH,
        )

    def send(cond, kind, i, ends, to, got=None):
        make(kind, i, *ends(), to, got).start()
        done = lambda: make(kind, i, *ends(), to, got).wait_send()
        if kind in ("sx", "sy"):
            staged[kind, i] = done
        else:
            sent.append((cond, done))

    def arrive(kind, i, dst, to):
        make(kind, i, dst, dst, to).wait_recv()

    def when(cond, body):
        pl.when(cond)(body)

    loads = [
        pltpu.make_async_copy(wg_hbm.at[0], wgv, load_sem.at[2]),
        pltpu.make_async_copy(wu_hbm.at[0], wuv, load_sem.at[3]),
        pltpu.make_async_copy(wd_hbm.at[0], wdv, load_sem.at[4]),
    ]

    def own_lists():
        return [
            pltpu.make_async_copy(ids_hbm, ids_ref, load_sem.at[5]),
            pltpu.make_async_copy(prob_hbm, prob_ref, load_sem.at[6]),
        ]

    def own_copies():
        return [
            pltpu.make_async_copy(x_hbm.at[:, pl.ds(0, 2 * near)], raw.at[z, 0], load_sem.at[0]),
            pltpu.make_async_copy(g_hbm.at[:, pl.ds(0, 2 * near)], raw.at[z, 1], load_sem.at[1]),
            pltpu.make_async_copy(x_hbm.at[:, av], rawv.at[z, 0, 0], load_sem.at[7]),
            pltpu.make_async_copy(g_hbm.at[:, av], rawv.at[z, 0, 1], load_sem.at[8]),
        ]

    def begin():
        for copy in own_lists() + own_copies():
            copy.start()

    when(ad, begin)
    for copy in loads:
        copy.start()

    barrier = pltpu.get_barrier_semaphore()
    greeted = [to_x, to_y, to_core]
    greeted += column[1:]
    for other in greeted:
        pl.semaphore_signal(barrier, inc=1, device_id=other, device_id_type=MESH)

    def table():
        for copy in own_lists():
            copy.wait()
        name = lax.broadcasted_iota(jnp.int32, (rows, 128), 1)
        count = jnp.zeros((rows, 128), f32)
        prob = jnp.zeros((rows, 128), f32)
        for k in range(ids_ref.shape[1]):
            hit = ids_ref[:, k:k + 1] == name
            count = count + jnp.where(hit, 1.0, 0.0)
            prob = prob + jnp.where(hit, prob_ref[:, k:k + 1], 0.0)
        before = lax.broadcasted_iota(jnp.int32, (rows, rows), 1) < lax.broadcasted_iota(jnp.int32, (rows, rows), 0)
        lower = jnp.where(before, 1.0, 0.0).astype(bf16)
        rank = jnp.dot(lower, count.astype(bf16), preferred_element_type=f32)
        code = jnp.where(count > 0.5, rank, -1.0)
        tabs[z, 0, 0:experts, :] = code.T[0:experts]
        tabs[z, 0, experts:, :] = prob.T[0:experts]

    def ready():
        for copy in own_copies():
            copy.wait()

    pl.semaphore_wait(barrier, len(greeted))
    when(ad, ready)

    def gather_z(i, cond):
        s = source[i]

        def body():
            n = jnp.where(s < z, 0, planes) + s
            arrive("tu", n, tabs.at[s, 0], column[i])
            arrive("ru", n, raw.at[s], column[i])

        if i > 0:
            when(cond, body)

    def pass_z(i, cond, names="tr"):
        s = source[i]
        go_up = cond & (s <= z) & (z < planes - 1)
        go_down = cond & (s >= z) & (z > 0)

        def up(names):
            if "t" in names:
                send(go_up, "tu", s, lambda: (tabs.at[s, 0], tabs.at[s, 0]), above)
            if "r" in names:
                send(go_up, "ru", s, lambda: (raw.at[s], raw.at[s]), above)

        def down(names):
            if "t" in names:
                send(go_down, "td", s, lambda: (tabs.at[s, 0], tabs.at[s, 0]), below)
            if "r" in names:
                send(go_down, "rd", s, lambda: (raw.at[s], raw.at[s]), below)

        when(go_up, lambda: up(names))
        when(go_down, lambda: down(names))

    def spread_table(i):
        s = source[i]

        def body():
            send(ad, "tx", i, lambda: (tabs.at[s, 0], tabs.at[s, 0]), to_x)
            send(ad, "ty", i, lambda: (tabs.at[s, 0], tabs.at[s, 1]), to_y)

        when(ad, body)

    def spread(i):
        s = source[i]

        def body():
            send(ad, "rx", i, lambda: (raw.at[s, :, :, a0], raw.at[s, :, :, a0]), to_x)
            send(ad, "ry", i, lambda: (raw.at[s, :, :, a1], raw.at[s, :, :, a1]), to_y)

        if i > 0:
            spread_table(i)
        when(ad, body)

    slot = lax.broadcasted_iota(jnp.int32, (cap, rows), 0).astype(f32)

    def build(i, h, t, target):
        s = source[i]
        for n, e in ((0, target), (1, me)):
            a = jnp.where(slot == tabs[s, t, pl.ds(e, 1), :], 1.0, 0.0)
            sel[i, h, n * cap:(n + 1) * cap, :] = a.astype(bf16)
            selt[i, h, n] = a.T.astype(bf16)

    step = cut // 2 if cut % 256 == 0 else cut

    def pack(i, h, to_rows):
        s = source[i]
        picker = sel[i, h]

        span = near // 2 if near % 256 == 0 else near

        @pl.loop(0, near // span)
        def _(n):
            local = pl.ds(pl.multiple_of(n * span, 128), span)
            cols = pl.ds(pl.multiple_of(h * near + n * span, 128), span)
            for k in range(2):
                picked = jnp.dot(picker, raw[s, k, :, cols], preferred_element_type=f32).astype(bf16)
                stage[i % 2, h, k, :, local] = picked[0:cap]
                comp[i, k, to_rows, cols] = picked[cap:]

    def plane_out(i):
        def body():
            send(ad, "vx", i, lambda: (rawv.at[z, 0], rawv.at[z, 0]), to_x)
            send(ad, "vy", i, lambda: (rawv.at[z, 0], rawv.at[z, 1]), to_y)

        when(ad, body)

    def plane_on(i):
        def left(k):
            return rawv.at[z, k, :, :, pl.ds(0, aside // 2)]

        def right(k):
            return rawv.at[z, k, :, :, pl.ds(aside // 2, aside // 2)]

        def body():
            arrive("vx", i, rawv.at[z, 0], to_x)
            send(bc, "wy", i, lambda: (left(0), left(1)), to_y)
            arrive("vy", i, rawv.at[z, 1], to_y)
            send(bc, "wx", i, lambda: (right(1), right(1)), to_x)

        when(bc, body)

    def diagonal_in(i):
        def body():
            arrive("wy", i, rawv.at[z, 1, :, :, pl.ds(0, aside // 2)], to_y)
            arrive("wx", i, rawv.at[z, 1, :, :, pl.ds(aside // 2, aside // 2)], to_x)
            arrive("t2", i, tabs.at[z, 1], to_y)

        when(ad, body)

    def pass_v(i, k):
        s = source[i]
        kind, kept = ("va", "vb")[k], ("ea", "eb")[k]
        place = {0: 0, 2: 1, 3: 2}.get(i)

        def on():
            got = jnp.where(outer, 1, 2) if i == 0 else 3
            make(kind, i, rawv.at[s, k], rawv.at[s, k], toward, got).start()

        def on_done():
            make(kind, i, rawv.at[s, k], rawv.at[s, k], toward, 0).wait_send()

        if i == 0:
            on()
            sent.append((None, on_done))
        elif i == 1:
            on()
            sent.append((inner, on_done))
        mine = jnp.where(slot == tabs[s, k, pl.ds(me, 1), :], 1.0, 0.0).astype(bf16)
        picker = mine
        if place is not None:
            theirs = jnp.where(slot == tabs[s, k, pl.ds(end, 1), :], 1.0, 0.0).astype(bf16)
            picker = jnp.concatenate([mine, theirs], axis=0)
        for n in range(2):
            picked = jnp.dot(picker, rawv[s, k, n], preferred_element_type=f32).astype(bf16)
            comp[i, n, slots[k], av] = picked[0:cap]
            if place is not None:
                stagev[place, k, n] = picked[cap:]

        def out():
            there = max(i, 1)
            send(inner, kept, i, lambda: (stagev.at[place, k], comp.at[there, :, slots[k], av]), to_end, got=there)

        if place is not None:
            when(inner, out)

    def relay_v(i, k):
        s = source[i]

        def body():
            arrive(("va", "vb")[k], i, rawv.at[s, k], toward)
            if k == 1:
                when(ad, lambda: arrive("t2", i, tabs.at[s, 1], to_y))
            pass_v(i, k)

        when(inner, body)

    def share_y(i):
        s = source[i]
        if i >= 2:
            staged.pop(("sy", i - 2))()

        def first():
            arrive("tx", i, tabs.at[s, 0], to_x)
            send(bc, "t2", i, lambda: (tabs.at[s, 0], tabs.at[s, 1]), to_y)
            arrive("rx", i, raw.at[s, :, :, a0], to_x)

        when(bc, first)
        build(i, 0, 0, peer_y)
        pack(i, 0, lo)
        send(None, "sy", i, lambda: (stage.at[i % 2, 0], comp.at[i, :, hi, a0]), to_y)

    def share_x(i):
        s = source[i]
        if i >= 2:
            staged.pop(("sx", i - 2))()

        def second():
            arrive("ty", i, tabs.at[s, 1], to_y)
            arrive("ry", i, raw.at[s, :, :, a1], to_y)

        when(bc, second)
        build(i, 1, tab1, peer_x)
        pack(i, 1, own1)
        send(None, "sx", i, lambda: (stage.at[i % 2, 1], comp.at[i, :, own1, a1]), to_x)

    def forward(i):
        s = source[i]
        arrive("sy", i, comp.at[i, :, hi, a0], to_y)
        arrive("sx", i, comp.at[i, :, other1, a1], to_x)
        if i > 0:
            when(ad & outer, lambda: arrive("t2", i, tabs.at[s, 1], to_y))
            for k in range(2):
                when(outer, lambda k=k: arrive(("ea", "eb")[k], i, comp.at[i, :, slots[k], av], to_end))
        for k in range(2):
            hit = slot == tabs[s, k, pl.ds(me, 1), :]
            pw[i, k * cap:(k + 1) * cap, :] = jnp.sum(
                jnp.where(hit, tabs[s, k, pl.ds(experts + me, 1), :], 0.0), axis=1, keepdims=True)
        tile = 256

        @pl.loop(0, hidden // tile)
        def _(f):
            cols = pl.ds(pl.multiple_of(f * tile, tile), tile)
            gate = jnp.dot(comp[i, 0], wgv[:, cols], preferred_element_type=f32)
            up = jnp.dot(comp[i, 0], wuv[:, cols], preferred_element_type=f32)
            grad = lax.dot_general(comp[i, 1], wdv[cols, :], NT, preferred_element_type=f32)
            s = jax.nn.sigmoid(gate)
            gg[i, :, cols] = (grad * up * s * (1.0 + gate * (1.0 - s))).astype(bf16)
            ug[i, :, cols] = (grad * gate * s).astype(bf16)

    def backward(i, h):
        @pl.loop(0, cut // step)
        def _(d):
            cols = pl.ds(pl.multiple_of(h * cut + d * step, 128), step)
            back = lax.dot_general(gg[i], wgv[cols, :], NT, preferred_element_type=f32)
            back = back + lax.dot_general(ug[i], wuv[cols, :], NT, preferred_element_type=f32)
            part[i, :, cols] = (back * pw[i]).astype(bf16)

    def back1_y(i):
        send(None, "py", i, lambda: (part.at[i, hi, h0], rc.at[i, :, h0]), to_y)

    def back1_x(i):
        send(None, "px", i, lambda: (part.at[i, other1, h1], rc.at[i, :, h1]), to_x)

    def merged(i, h, n, mine):
        cols = pl.ds(pl.multiple_of(h * cut + n * step, 128), step)
        value = jnp.dot(selt[i, h, 1], part[i, mine, cols], preferred_element_type=f32)
        return cols, value + jnp.dot(selt[i, h, 0], rc[i, :, cols], preferred_element_type=f32)

    routes = (("py", to_y, "qx", to_x, h0, lo), ("px", to_x, "qy", to_y, h1, hi))

    def back2(i, h):
        kind, to, out, there, half, mine = routes[h]

        def body():
            arrive(kind, i, rc.at[i, :, half], to)

            @pl.loop(0, cut // step)
            def _(n):
                cols, value = merged(i, h, n, mine)
                rr[i, :, cols] = value.astype(bf16)

            send(bc, out, i, lambda: (rr.at[i, :, half], rr.at[i, :, half]), there)

        when(bc, body)

    def back3(i, h):
        s = source[i]
        kind, to, out, there, half, mine = routes[h]
        home = ("z0", "z1")[h]

        def body():
            arrive(kind, i, rc.at[i, :, half], to)
            arrive(out, i, rr.at[i, :, half], there)
            if i == 0:
                for j in range(1, planes):
                    arrive(home, source[j], r3.at[source[j], :, half], column[j])

            @pl.loop(0, cut // step)
            def _(n):
                cols, value = merged(i, h, n, lo)
                value = value + rr[i, :, cols].astype(f32)
                if i == 0:
                    for j in range(1, planes):
                        value = value + r3[source[j], :, cols].astype(f32)
                rr[i, :, cols] = value.astype(bf16)

            if i > 0:
                send(ad, home, s, lambda: (rr.at[i, :, half], r3.at[z, :, half]), column[i], got=z)

        when(ad, body)
        if i == 0:
            over = ad & (core != h)
            when(over, lambda: send(over, "dp", h, lambda: (rr.at[0, :, half], out_ref), to_core))

    ops = {
        "sp": spread,
        "gz": lambda i: (gather_z(i, ad), pass_z(i, ad, "tr" if i else "r")),
        "tb": lambda i: (when(ad, table), spread_table(0), pass_z(0, ad, "t")),
        "gi": lambda i: (gather_z(i, ad & inner), pass_z(i, ad & inner)),
        "go": lambda i: gather_z(i, ad & outer),
        "v0": plane_out, "v1": plane_on,
        "za": lambda i: pass_v(i, 0), "zb": lambda i: (diagonal_in(i), pass_v(i, 1)),
        "ra": lambda i: relay_v(i, 0), "rb": lambda i: relay_v(i, 1),
        "sy": share_y, "sx": share_x, "cf": forward,
        "ca": lambda i: backward(i, 0), "cb": lambda i: backward(i, 1),
        "1y": back1_y, "1x": back1_x,
        "2y": lambda i: back2(i, 0), "2x": lambda i: back2(i, 1),
        "3y": lambda i: back3(i, 0), "3x": lambda i: back3(i, 1),
    }
    for name, i in STEPS:
        if name == "cf":
            while loads:
                loads.pop().wait()
        ops[name](i)

    def finish():
        out_ref[...] = jnp.where(core == 0, rr[0, :, 0:cut], rr[0, :, cut:])

    when(ad, finish)
    when(bc, lambda: arrive("dp", core, out_ref, to_core))
    for wait in staged.values():
        wait()
    for cond, wait in sent:
        if cond is None:
            wait()
        else:
            when(cond, wait)


def fused(layer_input, out_grad, expert_ids, gate_probs, gate_proj, up_proj, down_proj):
    experts, halves = lax.axis_size("ep"), lax.axis_size("dp")
    rows, features = layer_input.shape
    hidden = gate_proj.shape[2]
    planes = experts // 4
    cap = capacity(experts, expert_ids.shape)
    cut, bf16, f32 = features // 2, jnp.bfloat16, jnp.float32
    vmem, hbm = pl.BlockSpec(memory_space=pltpu.VMEM), pl.BlockSpec(memory_space=pl.ANY)
    aside = put_aside(features)
    near = (features - aside) // 2
    count = 26 * planes
    return pl.pallas_call(
        functools.partial(kernel, cap),
        name="fused_backward",
        out_shape=jax.ShapeDtypeStruct((rows, cut), bf16),
        in_specs=[hbm] * 7,
        out_specs=vmem,
        scratch_shapes=[
            pltpu.VMEM((planes, 2, rows, 2 * near), bf16),
            pltpu.VMEM((planes, 2, 2, rows, aside), bf16),
            pltpu.VMEM((planes, 2, 2 * experts, rows), f32),
            pltpu.VMEM((2, 2, 2, cap, near), bf16),
            pltpu.VMEM((planes - 1, 2, 2, cap, aside), bf16),
            pltpu.VMEM((planes, 2, 2 * cap, features), bf16),
            pltpu.VMEM((planes, 2 * cap, features), bf16),
            pltpu.VMEM((planes, cap, features), bf16),
            pltpu.VMEM((planes, rows, features), bf16),
            pltpu.VMEM((planes, rows, features), bf16),
            pltpu.VMEM((planes, 2, 2 * cap, rows), bf16),
            pltpu.VMEM((planes, 2, 2, rows, cap), bf16),
            pltpu.VMEM((features, hidden), bf16),
            pltpu.VMEM((features, hidden), bf16),
            pltpu.VMEM((hidden, features), bf16),
            pltpu.VMEM((planes, 2 * cap, hidden), bf16),
            pltpu.VMEM((planes, 2 * cap, hidden), bf16),
            pltpu.VMEM((planes, 2 * cap, 1), f32),
            pltpu.VMEM(expert_ids.shape, jnp.int32),
            pltpu.VMEM(gate_probs.shape, f32),
            pltpu.SemaphoreType.DMA((count,)),
            pltpu.SemaphoreType.DMA((count,)),
            pltpu.SemaphoreType.DMA((9,)),
        ],
        compiler_params=pltpu.CompilerParams(
            collective_id=0, has_side_effects=True, vmem_limit_bytes=67043328
        ),
    )(layer_input, out_grad, expert_ids, gate_probs, gate_proj, up_proj, down_proj)


def put_aside(features):
    return 2 * features // 7 // 256 * 256


def capacity(experts, shape):
    return 5 * shape[0] * shape[1] // (4 * experts)


def dense(layer_input, out_grad, expert_ids, gate_probs, gate_proj, up_proj, down_proj):
    experts = lax.axis_size("ep")
    halves = lax.axis_size("dp")
    tok_rows, features = layer_input.shape
    half = tok_rows // halves
    core = lax.axis_index("dp")
    start = core * half
    mine_in = lax.dynamic_slice_in_dim(layer_input, start, half, 0)
    mine_grad = lax.dynamic_slice_in_dim(out_grad, start, half, 0)
    ids = lax.dynamic_slice_in_dim(expert_ids, start, half, 0)
    probs = lax.dynamic_slice_in_dim(gate_probs, start, half, 0)
    names = jnp.arange(experts, dtype=jnp.int32)
    table = jnp.sum(
        jnp.where(ids[None, :, :] == names[:, None, None], probs[None, :, :], 0.0), axis=2
    )
    weight = lax.all_to_all(table, "ep", split_axis=0, concat_axis=0, tiled=True).reshape(-1)
    in_rows = lax.all_gather(mine_in, "ep", axis=0, tiled=True)
    grad_rows = lax.all_gather(mine_grad, "ep", axis=0, tiled=True)
    gate_mat, up_mat, down_mat = (gate_proj[0], up_proj[0], down_proj[0])
    nt = (((1,), (1,)), ((), ()))
    gate_pre = jnp.dot(in_rows, gate_mat, preferred_element_type=jnp.float32)
    up_pre = jnp.dot(in_rows, up_mat, preferred_element_type=jnp.float32)
    hidden_grad = lax.dot_general(grad_rows, down_mat, nt, preferred_element_type=jnp.float32)
    s = jax.nn.sigmoid(gate_pre)
    gate_grad = (hidden_grad * up_pre * s * (1.0 + gate_pre * (1.0 - s))).astype(jnp.bfloat16)
    up_grad = (hidden_grad * gate_pre * s).astype(jnp.bfloat16)
    back = lax.dot_general(gate_grad, gate_mat, nt, preferred_element_type=jnp.float32)
    back = back + lax.dot_general(up_grad, up_mat, nt, preferred_element_type=jnp.float32)
    back = (back * weight[:, None]).astype(jnp.bfloat16)
    mine = lax.psum_scatter(back, "ep", scatter_dimension=0, tiled=True)
    return lax.all_to_all(mine, "dp", split_axis=1, concat_axis=0, tiled=True)


def body(*args):
    experts, halves = lax.axis_size("ep"), lax.axis_size("dp")
    rows, features = args[0].shape
    hidden = args[4].shape[2]
    cap = capacity(experts, args[2].shape)
    held = 2 * features * (LINE * (4 * rows + 7 * cap) + 3 * hidden + 6 * cap) + 16 * LINE * cap * hidden
    fits = held < 66 * 10**6 and halves == 2 and experts == 4 * LINE and cap % 16 == 0
    return (fused if fits else dense)(*args)


def solution(mesh):
    row = P("ep", None)
    mat = P("ep", None, None)
    return jax.shard_map(
        body, mesh=mesh, in_specs=(row, row, row, row, mat, mat, mat), out_specs=P("ep", "dp"), check_vma=False
    )
```

```python
import functools

import jax
import jax.numpy as jnp
from jax import lax
from jax.experimental import pallas as pl
from jax.experimental.pallas import tpu as pltpu
from jax.sharding import PartitionSpec as P

MESH = pl.DeviceIdType.MESH
NT = (((1,), (1,)), ((), ()))


LINE = 4

STEPS = (
    ("gz", 0), ("sp", 0), ("v0", 0), ("tb", 0), ("v1", 0), ("sx", 0), ("sy", 0), ("gz", 1), ("gi", 2),
    ("sp", 1), ("sx", 1), ("za", 0), ("sy", 1), ("zb", 0), ("cf", 0), ("go", 2), ("cb", 0),
    ("sp", 2), ("gi", 3), ("ra", 1), ("rb", 1), ("sx", 2), ("sy", 2), ("cf", 1), ("ca", 1),
    ("cb", 1), ("go", 3), ("sp", 3), ("ra", 2), ("rb", 2), ("sy", 3), ("sx", 3), ("cf", 2),
    ("1x", 1), ("ca", 2), ("1y", 2), ("1y", 1), ("cb", 2), ("2y", 2), ("1x", 2), ("ca", 0),
    ("2x", 2), ("rb", 3), ("2x", 1), ("2y", 1), ("ra", 3), ("cf", 3), ("3y", 2), ("cb", 3),
    ("ca", 3), ("3x", 2), ("1x", 3), ("2x", 3), ("1y", 3), ("2y", 3), ("1x", 0), ("2x", 0),
    ("3x", 1), ("1y", 0), ("3y", 1), ("2y", 0), ("3x", 3), ("3y", 3), ("3x", 0), ("3y", 0),
)


def kernel(cap, x_hbm, g_hbm, ids_hbm, prob_hbm, wg_hbm, wu_hbm, wd_hbm, out_ref,
           raw, rawv, tabs, stage, stagev, comp, part, rc, rr, r3, sel, selt, wgv, wuv, wdv, gg, ug, pw, ids_ref, prob_ref,
           send_sem, recv_sem, load_sem):
    me, core = lax.axis_index("ep"), lax.axis_index("dp")
    z, y, x = me // 4, (me // 2) % 2, me % 2
    planes, rows, features = comp.shape[0], raw.shape[2], comp.shape[3]
    hidden, experts = wgv.shape[1], tabs.shape[2] // 2
    cut = features // 2
    f32, bf16 = jnp.float32, jnp.bfloat16
    ad = core == (x + y) % 2
    bc = core != (x + y) % 2
    off1 = jnp.where(ad, 0, cap)
    tab1 = jnp.where(ad, 0, 1)
    inner = (z % (planes - 1)) != 0
    outer = (z % (planes - 1)) == 0
    far = z // 2
    source = [z, z + 1 - 2 * (z % 2), 2 - far, 3 * (1 - far)]
    peer_x, peer_y = z * 4 + y * 2 + (1 - x), z * 4 + (1 - y) * 2 + x
    to_x, to_y, to_core = {"ep": peer_x}, {"ep": peer_y}, {"dp": 1 - core}
    column = [{"ep": s * 4 + y * 2 + x} for s in source]
    above = {"ep": jnp.minimum(z + 1, planes - 1) * 4 + y * 2 + x}
    below = {"ep": jnp.maximum(z - 1, 0) * 4 + y * 2 + x}
    near, aside = raw.shape[3] // 2, rawv.shape[4]
    a0, a1, av = pl.ds(0, near), pl.ds(near, near), pl.ds(2 * near, aside)
    h0, h1 = pl.ds(0, cut), pl.ds(cut, cut)
    slots = (pl.ds(0, cap), pl.ds(cap, cap))
    end = (planes - 1) * far * 4 + y * 2 + x
    toward = {"ep": jnp.where(inner, 2 - far, 1 + far) * 4 + y * 2 + x}
    to_end = {"ep": end}
    lo, hi = pl.ds(0, cap), pl.ds(cap, cap)
    own1 = pl.ds(pl.multiple_of(off1, 16), cap)
    other1 = pl.ds(pl.multiple_of(cap - off1, 16), cap)

    kinds = ("ru", "rd", "tu", "td", "rx", "ry", "tx", "ty", "t2", "sx", "sy", "px", "py", "qx", "qy", "z0", "z1", "dp",
             "va", "vb", "ea", "eb", "vx", "vy", "wx", "wy")
    sent, staged = [], {}

    def number(kind, i):
        return kinds.index(kind) * planes + i

    def make(kind, i, src, dst, to, got=None):
        return pltpu.make_async_remote_copy(
            src_ref=src, dst_ref=dst, send_sem=send_sem.at[number(kind, i)],
            recv_sem=recv_sem.at[number(kind, i if got is None else got)],
            device_id=to, device_id_type=MESH,
        )

    def send(cond, kind, i, ends, to, got=None):
        make(kind, i, *ends(), to, got).start()
        done = lambda: make(kind, i, *ends(), to, got).wait_send()
        if kind in ("sx", "sy"):
            staged[kind, i] = done
        else:
            sent.append((cond, done))

    def arrive(kind, i, dst, to):
        make(kind, i, dst, dst, to).wait_recv()

    def when(cond, body):
        pl.when(cond)(body)

    loads = [
        pltpu.make_async_copy(wg_hbm.at[0], wgv, load_sem.at[2]),
        pltpu.make_async_copy(wu_hbm.at[0], wuv, load_sem.at[3]),
        pltpu.make_async_copy(wd_hbm.at[0], wdv, load_sem.at[4]),
    ]

    def own_lists():
        return [
            pltpu.make_async_copy(ids_hbm, ids_ref, load_sem.at[5]),
            pltpu.make_async_copy(prob_hbm, prob_ref, load_sem.at[6]),
        ]

    def own_copies():
        return [
            pltpu.make_async_copy(x_hbm.at[:, pl.ds(0, 2 * near)], raw.at[z, 0], load_sem.at[0]),
            pltpu.make_async_copy(g_hbm.at[:, pl.ds(0, 2 * near)], raw.at[z, 1], load_sem.at[1]),
            pltpu.make_async_copy(x_hbm.at[:, av], rawv.at[z, 0, 0], load_sem.at[7]),
            pltpu.make_async_copy(g_hbm.at[:, av], rawv.at[z, 0, 1], load_sem.at[8]),
        ]

    def begin():
        for copy in own_lists() + own_copies():
            copy.start()

    when(ad, begin)
    for copy in loads:
        copy.start()

    barrier = pltpu.get_barrier_semaphore()
    greeted = [to_x, to_y, to_core]
    greeted += column[1:]
    for other in greeted:
        pl.semaphore_signal(barrier, inc=1, device_id=other, device_id_type=MESH)

    def table():
        for copy in own_lists():
            copy.wait()
        name = lax.broadcasted_iota(jnp.int32, (experts, rows), 0)
        count = jnp.zeros((experts, rows), f32)
        prob = jnp.zeros((experts, rows), f32)
        for k in range(ids_ref.shape[0]):
            hit = ids_ref[k:k + 1, :] == name
            count = count + jnp.where(hit, 1.0, 0.0)
            prob = prob + jnp.where(hit, prob_ref[k:k + 1, :], 0.0)
        before = lax.broadcasted_iota(jnp.int32, (rows, rows), 0) < lax.broadcasted_iota(jnp.int32, (rows, rows), 1)
        upper = jnp.where(before, 1.0, 0.0).astype(bf16)
        rank = jnp.dot(count.astype(bf16), upper, preferred_element_type=f32)
        tabs[z, 0, 0:experts, :] = jnp.where(count > 0.5, rank, -1.0)
        tabs[z, 0, experts:, :] = prob

    def ready():
        for copy in own_copies():
            copy.wait()

    pl.semaphore_wait(barrier, len(greeted))
    when(ad, ready)

    def gather_z(i, cond):
        s = source[i]

        def body():
            n = jnp.where(s < z, 0, planes) + s
            arrive("tu", n, tabs.at[s, 0], column[i])
            arrive("ru", n, raw.at[s], column[i])

        if i > 0:
            when(cond, body)

    def pass_z(i, cond, names="tr"):
        s = source[i]
        go_up = cond & (s <= z) & (z < planes - 1)
        go_down = cond & (s >= z) & (z > 0)

        def up(names):
            if "t" in names:
                send(go_up, "tu", s, lambda: (tabs.at[s, 0], tabs.at[s, 0]), above)
            if "r" in names:
                send(go_up, "ru", s, lambda: (raw.at[s], raw.at[s]), above)

        def down(names):
            if "t" in names:
                send(go_down, "td", s, lambda: (tabs.at[s, 0], tabs.at[s, 0]), below)
            if "r" in names:
                send(go_down, "rd", s, lambda: (raw.at[s], raw.at[s]), below)

        when(go_up, lambda: up(names))
        when(go_down, lambda: down(names))

    def spread_table(i):
        s = source[i]

        def body():
            send(ad, "tx", i, lambda: (tabs.at[s, 0], tabs.at[s, 0]), to_x)
            send(ad, "ty", i, lambda: (tabs.at[s, 0], tabs.at[s, 1]), to_y)

        when(ad, body)

    def spread(i):
        s = source[i]

        def body():
            send(ad, "rx", i, lambda: (raw.at[s, :, :, a0], raw.at[s, :, :, a0]), to_x)
            send(ad, "ry", i, lambda: (raw.at[s, :, :, a1], raw.at[s, :, :, a1]), to_y)

        if i > 0:
            spread_table(i)
        when(ad, body)

    slot = lax.broadcasted_iota(jnp.int32, (cap, rows), 0).astype(f32)

    def build(i, h, t, target):
        s = source[i]
        for n, e in ((0, target), (1, me)):
            a = jnp.where(slot == tabs[s, t, pl.ds(e, 1), :], 1.0, 0.0)
            sel[i, h, n * cap:(n + 1) * cap, :] = a.astype(bf16)
            selt[i, h, n] = a.T.astype(bf16)

    step = cut // 2 if cut % 256 == 0 else cut

    def pack(i, h, to_rows):
        s = source[i]
        picker = sel[i, h]

        span = near // 2 if near % 256 == 0 else near

        @pl.loop(0, near // span)
        def _(n):
            local = pl.ds(pl.multiple_of(n * span, 128), span)
            cols = pl.ds(pl.multiple_of(h * near + n * span, 128), span)
            for k in range(2):
                picked = jnp.dot(picker, raw[s, k, :, cols], preferred_element_type=f32).astype(bf16)
                stage[i % 2, h, k, :, local] = picked[0:cap]
                comp[i, k, to_rows, cols] = picked[cap:]

    def plane_out(i):
        def body():
            send(ad, "vx", i, lambda: (rawv.at[z, 0], rawv.at[z, 0]), to_x)
            send(ad, "vy", i, lambda: (rawv.at[z, 0], rawv.at[z, 1]), to_y)

        when(ad, body)

    def plane_on(i):
        def left(k):
            return rawv.at[z, k, :, :, pl.ds(0, aside // 2)]

        def right(k):
            return rawv.at[z, k, :, :, pl.ds(aside // 2, aside // 2)]

        def body():
            arrive("vx", i, rawv.at[z, 0], to_x)
            send(bc, "wy", i, lambda: (left(0), left(1)), to_y)
            arrive("vy", i, rawv.at[z, 1], to_y)
            send(bc, "wx", i, lambda: (right(1), right(1)), to_x)

        when(bc, body)

    def diagonal_in(i):
        def body():
            arrive("wy", i, rawv.at[z, 1, :, :, pl.ds(0, aside // 2)], to_y)
            arrive("wx", i, rawv.at[z, 1, :, :, pl.ds(aside // 2, aside // 2)], to_x)
            arrive("t2", i, tabs.at[z, 1], to_y)

        when(ad, body)

    def pass_v(i, k):
        s = source[i]
        kind, kept = ("va", "vb")[k], ("ea", "eb")[k]
        place = {0: 0, 2: 1, 3: 2}.get(i)

        def on():
            got = jnp.where(outer, 1, 2) if i == 0 else 3
            make(kind, i, rawv.at[s, k], rawv.at[s, k], toward, got).start()

        def on_done():
            make(kind, i, rawv.at[s, k], rawv.at[s, k], toward, 0).wait_send()

        if i == 0:
            on()
            sent.append((None, on_done))
        elif i == 1:
            on()
            sent.append((inner, on_done))
        mine = jnp.where(slot == tabs[s, k, pl.ds(me, 1), :], 1.0, 0.0).astype(bf16)
        picker = mine
        if place is not None:
            theirs = jnp.where(slot == tabs[s, k, pl.ds(end, 1), :], 1.0, 0.0).astype(bf16)
            picker = jnp.concatenate([mine, theirs], axis=0)
        for n in range(2):
            picked = jnp.dot(picker, rawv[s, k, n], preferred_element_type=f32).astype(bf16)
            comp[i, n, slots[k], av] = picked[0:cap]
            if place is not None:
                stagev[place, k, n] = picked[cap:]

        def out():
            there = max(i, 1)
            send(inner, kept, i, lambda: (stagev.at[place, k], comp.at[there, :, slots[k], av]), to_end, got=there)

        if place is not None:
            when(inner, out)

    def relay_v(i, k):
        s = source[i]

        def body():
            arrive(("va", "vb")[k], i, rawv.at[s, k], toward)
            if k == 1:
                when(ad, lambda: arrive("t2", i, tabs.at[s, 1], to_y))
            pass_v(i, k)

        when(inner, body)

    def share_y(i):
        s = source[i]
        if i >= 2:
            staged.pop(("sy", i - 2))()

        def first():
            arrive("tx", i, tabs.at[s, 0], to_x)
            send(bc, "t2", i, lambda: (tabs.at[s, 0], tabs.at[s, 1]), to_y)
            arrive("rx", i, raw.at[s, :, :, a0], to_x)

        when(bc, first)
        build(i, 0, 0, peer_y)
        pack(i, 0, lo)
        send(None, "sy", i, lambda: (stage.at[i % 2, 0], comp.at[i, :, hi, a0]), to_y)

    def share_x(i):
        s = source[i]
        if i >= 2:
            staged.pop(("sx", i - 2))()

        def second():
            arrive("ty", i, tabs.at[s, 1], to_y)
            arrive("ry", i, raw.at[s, :, :, a1], to_y)

        when(bc, second)
        build(i, 1, tab1, peer_x)
        pack(i, 1, own1)
        send(None, "sx", i, lambda: (stage.at[i % 2, 1], comp.at[i, :, own1, a1]), to_x)

    def forward(i):
        s = source[i]
        arrive("sy", i, comp.at[i, :, hi, a0], to_y)
        arrive("sx", i, comp.at[i, :, other1, a1], to_x)
        if i > 0:
            when(ad & outer, lambda: arrive("t2", i, tabs.at[s, 1], to_y))
            for k in range(2):
                when(outer, lambda k=k: arrive(("ea", "eb")[k], i, comp.at[i, :, slots[k], av], to_end))
        for k in range(2):
            hit = slot == tabs[s, k, pl.ds(me, 1), :]
            pw[i, k * cap:(k + 1) * cap, :] = jnp.sum(
                jnp.where(hit, tabs[s, k, pl.ds(experts + me, 1), :], 0.0), axis=1, keepdims=True)
        tile = 256

        @pl.loop(0, hidden // tile)
        def _(f):
            cols = pl.ds(pl.multiple_of(f * tile, tile), tile)
            gate = jnp.dot(comp[i, 0], wgv[:, cols], preferred_element_type=f32)
            up = jnp.dot(comp[i, 0], wuv[:, cols], preferred_element_type=f32)
            grad = lax.dot_general(comp[i, 1], wdv[cols, :], NT, preferred_element_type=f32)
            s = jax.nn.sigmoid(gate)
            gg[i, :, cols] = (grad * up * s * (1.0 + gate * (1.0 - s))).astype(bf16)
            ug[i, :, cols] = (grad * gate * s).astype(bf16)

    def backward(i, h):
        @pl.loop(0, cut // step)
        def _(d):
            cols = pl.ds(pl.multiple_of(h * cut + d * step, 128), step)
            back = lax.dot_general(gg[i], wgv[cols, :], NT, preferred_element_type=f32)
            back = back + lax.dot_general(ug[i], wuv[cols, :], NT, preferred_element_type=f32)
            part[i, :, cols] = (back * pw[i]).astype(bf16)

    def back1_y(i):
        send(None, "py", i, lambda: (part.at[i, hi, h0], rc.at[i, :, h0]), to_y)

    def back1_x(i):
        send(None, "px", i, lambda: (part.at[i, other1, h1], rc.at[i, :, h1]), to_x)

    def merged(i, h, n, mine):
        cols = pl.ds(pl.multiple_of(h * cut + n * step, 128), step)
        value = jnp.dot(selt[i, h, 1], part[i, mine, cols], preferred_element_type=f32)
        return cols, value + jnp.dot(selt[i, h, 0], rc[i, :, cols], preferred_element_type=f32)

    routes = (("py", to_y, "qx", to_x, h0, lo), ("px", to_x, "qy", to_y, h1, hi))

    def back2(i, h):
        kind, to, out, there, half, mine = routes[h]

        def body():
            arrive(kind, i, rc.at[i, :, half], to)

            @pl.loop(0, cut // step)
            def _(n):
                cols, value = merged(i, h, n, mine)
                rr[i, :, cols] = value.astype(bf16)

            send(bc, out, i, lambda: (rr.at[i, :, half], rr.at[i, :, half]), there)

        when(bc, body)

    def back3(i, h):
        s = source[i]
        kind, to, out, there, half, mine = routes[h]
        home = ("z0", "z1")[h]

        def body():
            arrive(kind, i, rc.at[i, :, half], to)
            arrive(out, i, rr.at[i, :, half], there)
            if i == 0:
                for j in range(1, planes):
                    arrive(home, source[j], r3.at[source[j], :, half], column[j])

            @pl.loop(0, cut // step)
            def _(n):
                cols, value = merged(i, h, n, lo)
                value = value + rr[i, :, cols].astype(f32)
                if i == 0:
                    for j in range(1, planes):
                        value = value + r3[source[j], :, cols].astype(f32)
                rr[i, :, cols] = value.astype(bf16)

            if i > 0:
                send(ad, home, s, lambda: (rr.at[i, :, half], r3.at[z, :, half]), column[i], got=z)

        when(ad, body)
        if i == 0:
            over = ad & (core != h)
            when(over, lambda: send(over, "dp", h, lambda: (rr.at[0, :, half], out_ref), to_core))

    ops = {
        "sp": spread,
        "gz": lambda i: (gather_z(i, ad), pass_z(i, ad, "tr" if i else "r")),
        "tb": lambda i: (when(ad, table), spread_table(0), pass_z(0, ad, "t")),
        "gi": lambda i: (gather_z(i, ad & inner), pass_z(i, ad & inner)),
        "go": lambda i: gather_z(i, ad & outer),
        "v0": plane_out, "v1": plane_on,
        "za": lambda i: pass_v(i, 0), "zb": lambda i: (diagonal_in(i), pass_v(i, 1)),
        "ra": lambda i: relay_v(i, 0), "rb": lambda i: relay_v(i, 1),
        "sy": share_y, "sx": share_x, "cf": forward,
        "ca": lambda i: backward(i, 0), "cb": lambda i: backward(i, 1),
        "1y": back1_y, "1x": back1_x,
        "2y": lambda i: back2(i, 0), "2x": lambda i: back2(i, 1),
        "3y": lambda i: back3(i, 0), "3x": lambda i: back3(i, 1),
    }
    for name, i in STEPS:
        if name == "cf":
            while loads:
                loads.pop().wait()
        ops[name](i)

    def finish():
        out_ref[...] = jnp.where(core == 0, rr[0, :, 0:cut], rr[0, :, cut:])

    when(ad, finish)
    when(bc, lambda: arrive("dp", core, out_ref, to_core))
    for wait in staged.values():
        wait()
    for cond, wait in sent:
        if cond is None:
            wait()
        else:
            when(cond, wait)


def fused(layer_input, out_grad, expert_ids, gate_probs, gate_proj, up_proj, down_proj):
    experts, halves = lax.axis_size("ep"), lax.axis_size("dp")
    rows, features = layer_input.shape
    hidden = gate_proj.shape[2]
    planes = experts // 4
    cap = capacity(experts, expert_ids.shape)
    cut, bf16, f32 = features // 2, jnp.bfloat16, jnp.float32
    vmem, hbm = pl.BlockSpec(memory_space=pltpu.VMEM), pl.BlockSpec(memory_space=pl.ANY)
    aside = put_aside(features)
    near = (features - aside) // 2
    count = 26 * planes
    return pl.pallas_call(
        functools.partial(kernel, cap),
        name="fused_backward",
        out_shape=jax.ShapeDtypeStruct((rows, cut), bf16),
        in_specs=[hbm] * 7,
        out_specs=vmem,
        scratch_shapes=[
            pltpu.VMEM((planes, 2, rows, 2 * near), bf16),
            pltpu.VMEM((planes, 2, 2, rows, aside), bf16),
            pltpu.VMEM((planes, 2, 2 * experts, rows), f32),
            pltpu.VMEM((2, 2, 2, cap, near), bf16),
            pltpu.VMEM((planes - 1, 2, 2, cap, aside), bf16),
            pltpu.VMEM((planes, 2, 2 * cap, features), bf16),
            pltpu.VMEM((planes, 2 * cap, features), bf16),
            pltpu.VMEM((planes, cap, features), bf16),
            pltpu.VMEM((planes, rows, features), bf16),
            pltpu.VMEM((planes, rows, features), bf16),
            pltpu.VMEM((planes, 2, 2 * cap, rows), bf16),
            pltpu.VMEM((planes, 2, 2, rows, cap), bf16),
            pltpu.VMEM((features, hidden), bf16),
            pltpu.VMEM((features, hidden), bf16),
            pltpu.VMEM((hidden, features), bf16),
            pltpu.VMEM((planes, 2 * cap, hidden), bf16),
            pltpu.VMEM((planes, 2 * cap, hidden), bf16),
            pltpu.VMEM((planes, 2 * cap, 1), f32),
            pltpu.VMEM(expert_ids.shape[::-1], jnp.int32),
            pltpu.VMEM(gate_probs.shape[::-1], f32),
            pltpu.SemaphoreType.DMA((count,)),
            pltpu.SemaphoreType.DMA((count,)),
            pltpu.SemaphoreType.DMA((9,)),
        ],
        compiler_params=pltpu.CompilerParams(
            collective_id=0, has_side_effects=True, vmem_limit_bytes=67043328
        ),
    )(layer_input, out_grad, expert_ids.T, gate_probs.T, gate_proj, up_proj, down_proj)


def put_aside(features):
    return 2 * features // 7 // 256 * 256


def capacity(experts, shape):
    return 5 * shape[0] * shape[1] // (4 * experts)


def dense(layer_input, out_grad, expert_ids, gate_probs, gate_proj, up_proj, down_proj):
    experts = lax.axis_size("ep")
    halves = lax.axis_size("dp")
    tok_rows, features = layer_input.shape
    half = tok_rows // halves
    core = lax.axis_index("dp")
    start = core * half
    mine_in = lax.dynamic_slice_in_dim(layer_input, start, half, 0)
    mine_grad = lax.dynamic_slice_in_dim(out_grad, start, half, 0)
    ids = lax.dynamic_slice_in_dim(expert_ids, start, half, 0)
    probs = lax.dynamic_slice_in_dim(gate_probs, start, half, 0)
    names = jnp.arange(experts, dtype=jnp.int32)
    table = jnp.sum(
        jnp.where(ids[None, :, :] == names[:, None, None], probs[None, :, :], 0.0), axis=2
    )
    weight = lax.all_to_all(table, "ep", split_axis=0, concat_axis=0, tiled=True).reshape(-1)
    in_rows = lax.all_gather(mine_in, "ep", axis=0, tiled=True)
    grad_rows = lax.all_gather(mine_grad, "ep", axis=0, tiled=True)
    gate_mat, up_mat, down_mat = (gate_proj[0], up_proj[0], down_proj[0])
    nt = (((1,), (1,)), ((), ()))
    gate_pre = jnp.dot(in_rows, gate_mat, preferred_element_type=jnp.float32)
    up_pre = jnp.dot(in_rows, up_mat, preferred_element_type=jnp.float32)
    hidden_grad = lax.dot_general(grad_rows, down_mat, nt, preferred_element_type=jnp.float32)
    s = jax.nn.sigmoid(gate_pre)
    gate_grad = (hidden_grad * up_pre * s * (1.0 + gate_pre * (1.0 - s))).astype(jnp.bfloat16)
    up_grad = (hidden_grad * gate_pre * s).astype(jnp.bfloat16)
    back = lax.dot_general(gate_grad, gate_mat, nt, preferred_element_type=jnp.float32)
    back = back + lax.dot_general(up_grad, up_mat, nt, preferred_element_type=jnp.float32)
    back = (back * weight[:, None]).astype(jnp.bfloat16)
    mine = lax.psum_scatter(back, "ep", scatter_dimension=0, tiled=True)
    return lax.all_to_all(mine, "dp", split_axis=1, concat_axis=0, tiled=True)


def body(*args):
    experts, halves = lax.axis_size("ep"), lax.axis_size("dp")
    rows, features = args[0].shape
    hidden = args[4].shape[2]
    cap = capacity(experts, args[2].shape)
    held = 2 * features * (LINE * (4 * rows + 7 * cap) + 3 * hidden + 6 * cap) + 16 * LINE * cap * hidden
    fits = held < 66 * 10**6 and halves == 2 and experts == 4 * LINE and cap % 16 == 0
    return (fused if fits else dense)(*args)


def solution(mesh):
    row = P("ep", None)
    mat = P("ep", None, None)
    return jax.shard_map(
        body, mesh=mesh, in_specs=(row, row, row, row, mat, mat, mat), out_specs=P("ep", "dp"), check_vma=False
    )
```

```python
import functools

import jax
import jax.numpy as jnp
from jax import lax
from jax.experimental import pallas as pl
from jax.experimental.pallas import tpu as pltpu
from jax.sharding import PartitionSpec as P

MESH = pl.DeviceIdType.MESH
NT = (((1,), (1,)), ((), ()))


LINE = 4

STEPS = (
    ("gz", 0), ("sp", 0), ("v0", 0), ("tb", 0), ("v1", 0), ("sx", 0), ("sy", 0), ("gz", 1), ("gi", 2),
    ("sp", 1), ("sx", 1), ("za", 0), ("sy", 1), ("zb", 0), ("cf", 0), ("go", 2), ("cb", 0),
    ("sp", 2), ("gi", 3), ("ra", 1), ("rb", 1), ("sx", 2), ("sy", 2), ("cf", 1), ("ca", 1),
    ("cb", 1), ("go", 3), ("sp", 3), ("ra", 2), ("rb", 2), ("sy", 3), ("sx", 3), ("cf", 2),
    ("1x", 1), ("ca", 2), ("1y", 2), ("1y", 1), ("cb", 2), ("2y", 2), ("1x", 2), ("ca", 0),
    ("2x", 2), ("rb", 3), ("2x", 1), ("2y", 1), ("ra", 3), ("cf", 3), ("3y", 2), ("cb", 3),
    ("ca", 3), ("3x", 2), ("1x", 3), ("2x", 3), ("1y", 3), ("2y", 3), ("1x", 0), ("2x", 0),
    ("3x", 1), ("1y", 0), ("3y", 1), ("2y", 0), ("3x", 3), ("3y", 3), ("3x", 0), ("3y", 0),
)


def kernel(cap, x_hbm, g_hbm, ids_hbm, prob_hbm, wg_hbm, wu_hbm, wd_hbm, out_ref,
           raw, rawv, tabs, stage, stagev, comp, part, rc, rr, r3, sel, selt, wgv, wuv, wdv, gg, ug, pw, ids_ref, prob_ref,
           send_sem, recv_sem, load_sem):
    me, core = lax.axis_index("ep"), lax.axis_index("dp")
    z, y, x = me // 4, (me // 2) % 2, me % 2
    planes, rows, features = comp.shape[0], raw.shape[2], comp.shape[3]
    hidden, experts = wgv.shape[1], tabs.shape[2] // 2
    cut = features // 2
    f32, bf16 = jnp.float32, jnp.bfloat16
    ad = core == (x + y) % 2
    bc = core != (x + y) % 2
    off1 = jnp.where(ad, 0, cap)
    tab1 = jnp.where(ad, 0, 1)
    inner = (z % (planes - 1)) != 0
    outer = (z % (planes - 1)) == 0
    far = z // 2
    source = [z, z + 1 - 2 * (z % 2), 2 - far, 3 * (1 - far)]
    peer_x, peer_y = z * 4 + y * 2 + (1 - x), z * 4 + (1 - y) * 2 + x
    to_x, to_y, to_core = {"ep": peer_x}, {"ep": peer_y}, {"dp": 1 - core}
    column = [{"ep": s * 4 + y * 2 + x} for s in source]
    above = {"ep": jnp.minimum(z + 1, planes - 1) * 4 + y * 2 + x}
    below = {"ep": jnp.maximum(z - 1, 0) * 4 + y * 2 + x}
    near, aside = raw.shape[3] // 2, rawv.shape[4]
    a0, a1, av = pl.ds(0, near), pl.ds(near, near), pl.ds(2 * near, aside)
    h0, h1 = pl.ds(0, cut), pl.ds(cut, cut)
    slots = (pl.ds(0, cap), pl.ds(cap, cap))
    end = (planes - 1) * far * 4 + y * 2 + x
    toward = {"ep": jnp.where(inner, 2 - far, 1 + far) * 4 + y * 2 + x}
    to_end = {"ep": end}
    lo, hi = pl.ds(0, cap), pl.ds(cap, cap)
    own1 = pl.ds(pl.multiple_of(off1, 16), cap)
    other1 = pl.ds(pl.multiple_of(cap - off1, 16), cap)

    kinds = ("ru", "rd", "tu", "td", "rx", "ry", "tx", "ty", "t2", "sx", "sy", "px", "py", "qx", "qy", "z0", "z1", "dp",
             "va", "vb", "ea", "eb", "vx", "vy", "wx", "wy")
    sent, staged = [], {}

    def number(kind, i):
        return kinds.index(kind) * planes + i

    def make(kind, i, src, dst, to, got=None):
        return pltpu.make_async_remote_copy(
            src_ref=src, dst_ref=dst, send_sem=send_sem.at[number(kind, i)],
            recv_sem=recv_sem.at[number(kind, i if got is None else got)],
            device_id=to, device_id_type=MESH,
        )

    def send(cond, kind, i, ends, to, got=None):
        make(kind, i, *ends(), to, got).start()
        done = lambda: make(kind, i, *ends(), to, got).wait_send()
        if kind in ("sx", "sy"):
            staged[kind, i] = done
        else:
            sent.append((cond, done))

    def arrive(kind, i, dst, to):
        make(kind, i, dst, dst, to).wait_recv()

    def when(cond, body):
        pl.when(cond)(body)

    loads = [
        pltpu.make_async_copy(wg_hbm.at[0], wgv, load_sem.at[2]),
        pltpu.make_async_copy(wu_hbm.at[0], wuv, load_sem.at[3]),
        pltpu.make_async_copy(wd_hbm.at[0], wdv, load_sem.at[4]),
    ]

    def own_lists():
        return [
            pltpu.make_async_copy(ids_hbm, ids_ref, load_sem.at[5]),
            pltpu.make_async_copy(prob_hbm, prob_ref, load_sem.at[6]),
        ]

    def own_copies():
        return [
            pltpu.make_async_copy(x_hbm.at[:, pl.ds(0, 2 * near)], raw.at[z, 0], load_sem.at[0]),
            pltpu.make_async_copy(g_hbm.at[:, pl.ds(0, 2 * near)], raw.at[z, 1], load_sem.at[1]),
            pltpu.make_async_copy(x_hbm.at[:, av], rawv.at[z, 0, 0], load_sem.at[7]),
            pltpu.make_async_copy(g_hbm.at[:, av], rawv.at[z, 0, 1], load_sem.at[8]),
        ]

    def begin():
        for copy in own_lists() + own_copies():
            copy.start()

    when(ad, begin)
    for copy in loads:
        copy.start()

    barrier = pltpu.get_barrier_semaphore()
    greeted = [to_x, to_y, to_core]
    greeted += column[1:]
    for other in greeted:
        pl.semaphore_signal(barrier, inc=1, device_id=other, device_id_type=MESH)

    def table():
        for copy in own_lists():
            copy.wait()
        name = lax.broadcasted_iota(jnp.int32, (experts, rows), 0)
        count = jnp.zeros((experts, rows), f32)
        prob = jnp.zeros((experts, rows), f32)
        for k in range(ids_ref.shape[0]):
            hit = ids_ref[k:k + 1, :] == name
            count = count + jnp.where(hit, 1.0, 0.0)
            prob = prob + jnp.where(hit, prob_ref[k:k + 1, :], 0.0)
        before = lax.broadcasted_iota(jnp.int32, (rows, rows), 0) < lax.broadcasted_iota(jnp.int32, (rows, rows), 1)
        upper = jnp.where(before, 1.0, 0.0).astype(bf16)
        rank = jnp.dot(count.astype(bf16), upper, preferred_element_type=f32)
        tabs[z, 0, 0:experts, :] = jnp.where(count > 0.5, rank, -1.0)
        tabs[z, 0, experts:, :] = prob

    def ready():
        for copy in own_copies():
            copy.wait()

    pl.semaphore_wait(barrier, len(greeted))
    when(ad, ready)

    def gather_z(i, cond):
        s = source[i]

        def body():
            n = jnp.where(s < z, 0, planes) + s
            arrive("tu", n, tabs.at[s, 0], column[i])
            arrive("ru", n, raw.at[s], column[i])

        if i > 0:
            when(cond, body)

    def pass_z(i, cond, names="tr"):
        s = source[i]
        go_up = cond & (s <= z) & (z < planes - 1)
        go_down = cond & (s >= z) & (z > 0)

        def up(names):
            if "t" in names:
                send(go_up, "tu", s, lambda: (tabs.at[s, 0], tabs.at[s, 0]), above)
            if "r" in names:
                send(go_up, "ru", s, lambda: (raw.at[s], raw.at[s]), above)

        def down(names):
            if "t" in names:
                send(go_down, "td", s, lambda: (tabs.at[s, 0], tabs.at[s, 0]), below)
            if "r" in names:
                send(go_down, "rd", s, lambda: (raw.at[s], raw.at[s]), below)

        when(go_up, lambda: up(names))
        when(go_down, lambda: down(names))

    def spread_table(i):
        s = source[i]

        def body():
            send(ad, "tx", i, lambda: (tabs.at[s, 0], tabs.at[s, 0]), to_x)
            send(ad, "ty", i, lambda: (tabs.at[s, 0], tabs.at[s, 1]), to_y)

        when(ad, body)

    def spread(i):
        s = source[i]

        def body():
            send(ad, "rx", i, lambda: (raw.at[s, :, :, a0], raw.at[s, :, :, a0]), to_x)
            send(ad, "ry", i, lambda: (raw.at[s, :, :, a1], raw.at[s, :, :, a1]), to_y)

        if i > 0:
            spread_table(i)
        when(ad, body)

    slot = lax.broadcasted_iota(jnp.int32, (cap, rows), 0).astype(f32)

    def build(i, h, t, target):
        s = source[i]
        for n, e in ((0, target), (1, me)):
            a = jnp.where(slot == tabs[s, t, pl.ds(e, 1), :], 1.0, 0.0)
            sel[i, h, n * cap:(n + 1) * cap, :] = a.astype(bf16)
            selt[i, h, n] = a.T.astype(bf16)

    step = cut // 2 if cut % 256 == 0 else cut

    def pack(i, h, to_rows):
        s = source[i]
        picker = sel[i, h]

        span = near // 2 if near % 256 == 0 else near

        @pl.loop(0, near // span)
        def _(n):
            local = pl.ds(pl.multiple_of(n * span, 128), span)
            cols = pl.ds(pl.multiple_of(h * near + n * span, 128), span)
            for k in range(2):
                picked = jnp.dot(picker, raw[s, k, :, cols], preferred_element_type=f32).astype(bf16)
                stage[i % 2, h, k, :, local] = picked[0:cap]
                comp[i, k, to_rows, cols] = picked[cap:]

    def plane_out(i):
        def body():
            send(ad, "vx", i, lambda: (rawv.at[z, 0], rawv.at[z, 0]), to_x)
            send(ad, "vy", i, lambda: (rawv.at[z, 0], rawv.at[z, 1]), to_y)

        when(ad, body)

    def plane_on(i):
        def left(k):
            return rawv.at[z, k, :, :, pl.ds(0, aside // 2)]

        def right(k):
            return rawv.at[z, k, :, :, pl.ds(aside // 2, aside // 2)]

        def body():
            arrive("vx", i, rawv.at[z, 0], to_x)
            send(bc, "wy", i, lambda: (left(0), left(1)), to_y)
            arrive("vy", i, rawv.at[z, 1], to_y)
            send(bc, "wx", i, lambda: (right(1), right(1)), to_x)

        when(bc, body)

    def diagonal_in(i):
        def body():
            arrive("wy", i, rawv.at[z, 1, :, :, pl.ds(0, aside // 2)], to_y)
            arrive("wx", i, rawv.at[z, 1, :, :, pl.ds(aside // 2, aside // 2)], to_x)
            arrive("t2", i, tabs.at[z, 1], to_y)

        when(ad, body)

    def pass_v(i, k):
        s = source[i]
        kind, kept = ("va", "vb")[k], ("ea", "eb")[k]
        place = {0: 0, 2: 1, 3: 2}.get(i)

        def on():
            got = jnp.where(outer, 1, 2) if i == 0 else 3
            make(kind, i, rawv.at[s, k], rawv.at[s, k], toward, got).start()

        def on_done():
            make(kind, i, rawv.at[s, k], rawv.at[s, k], toward, 0).wait_send()

        if i == 0:
            on()
            sent.append((None, on_done))
        elif i == 1:
            on()
            sent.append((inner, on_done))
        mine = jnp.where(slot == tabs[s, k, pl.ds(me, 1), :], 1.0, 0.0).astype(bf16)
        picker = mine
        if place is not None:
            theirs = jnp.where(slot == tabs[s, k, pl.ds(end, 1), :], 1.0, 0.0).astype(bf16)
            picker = jnp.concatenate([mine, theirs], axis=0)
        for n in range(2):
            picked = jnp.dot(picker, rawv[s, k, n], preferred_element_type=f32).astype(bf16)
            comp[i, n, slots[k], av] = picked[0:cap]
            if place is not None:
                stagev[place, k, n] = picked[cap:]

        def out():
            there = max(i, 1)
            send(inner, kept, i, lambda: (stagev.at[place, k], comp.at[there, :, slots[k], av]), to_end, got=there)

        if place is not None:
            when(inner, out)

    def relay_v(i, k):
        s = source[i]

        def body():
            arrive(("va", "vb")[k], i, rawv.at[s, k], toward)
            if k == 1:
                when(ad, lambda: arrive("t2", i, tabs.at[s, 1], to_y))
            pass_v(i, k)

        when(inner, body)

    def share_y(i):
        s = source[i]
        if i >= 2:
            staged.pop(("sy", i - 2))()

        def first():
            arrive("tx", i, tabs.at[s, 0], to_x)
            send(bc, "t2", i, lambda: (tabs.at[s, 0], tabs.at[s, 1]), to_y)
            arrive("rx", i, raw.at[s, :, :, a0], to_x)

        when(bc, first)
        build(i, 0, 0, peer_y)
        pack(i, 0, lo)
        send(None, "sy", i, lambda: (stage.at[i % 2, 0], comp.at[i, :, hi, a0]), to_y)

    def share_x(i):
        s = source[i]
        if i >= 2:
            staged.pop(("sx", i - 2))()

        def second():
            arrive("ty", i, tabs.at[s, 1], to_y)
            arrive("ry", i, raw.at[s, :, :, a1], to_y)

        when(bc, second)
        build(i, 1, tab1, peer_x)
        pack(i, 1, own1)
        send(None, "sx", i, lambda: (stage.at[i % 2, 1], comp.at[i, :, own1, a1]), to_x)

    def forward(i):
        s = source[i]
        arrive("sy", i, comp.at[i, :, hi, a0], to_y)
        arrive("sx", i, comp.at[i, :, other1, a1], to_x)
        if i > 0:
            when(ad & outer, lambda: arrive("t2", i, tabs.at[s, 1], to_y))
            for k in range(2):
                when(outer, lambda k=k: arrive(("ea", "eb")[k], i, comp.at[i, :, slots[k], av], to_end))
        for k in range(2):
            hit = slot == tabs[s, k, pl.ds(me, 1), :]
            pw[i, k * cap:(k + 1) * cap, :] = jnp.sum(
                jnp.where(hit, tabs[s, k, pl.ds(experts + me, 1), :], 0.0), axis=1, keepdims=True)
        tile = min(512, hidden)

        @pl.loop(0, hidden // tile)
        def _(f):
            cols = pl.ds(pl.multiple_of(f * tile, tile), tile)
            gate = jnp.dot(comp[i, 0], wgv[:, cols], preferred_element_type=f32)
            up = jnp.dot(comp[i, 0], wuv[:, cols], preferred_element_type=f32)
            grad = lax.dot_general(comp[i, 1], wdv[cols, :], NT, preferred_element_type=f32)
            s = jax.nn.sigmoid(gate)
            gg[i, :, cols] = (grad * up * s * (1.0 + gate * (1.0 - s))).astype(bf16)
            ug[i, :, cols] = (grad * gate * s).astype(bf16)

    def backward(i, h):
        @pl.loop(0, cut // step)
        def _(d):
            cols = pl.ds(pl.multiple_of(h * cut + d * step, 128), step)
            back = lax.dot_general(gg[i], wgv[cols, :], NT, preferred_element_type=f32)
            back = back + lax.dot_general(ug[i], wuv[cols, :], NT, preferred_element_type=f32)
            part[i, :, cols] = (back * pw[i]).astype(bf16)

    def back1_y(i):
        send(None, "py", i, lambda: (part.at[i, hi, h0], rc.at[i, :, h0]), to_y)

    def back1_x(i):
        send(None, "px", i, lambda: (part.at[i, other1, h1], rc.at[i, :, h1]), to_x)

    def merged(i, h, n, mine):
        cols = pl.ds(pl.multiple_of(h * cut + n * step, 128), step)
        value = jnp.dot(selt[i, h, 1], part[i, mine, cols], preferred_element_type=f32)
        return cols, value + jnp.dot(selt[i, h, 0], rc[i, :, cols], preferred_element_type=f32)

    routes = (("py", to_y, "qx", to_x, h0, lo), ("px", to_x, "qy", to_y, h1, hi))

    def back2(i, h):
        kind, to, out, there, half, mine = routes[h]

        def body():
            arrive(kind, i, rc.at[i, :, half], to)

            @pl.loop(0, cut // step)
            def _(n):
                cols, value = merged(i, h, n, mine)
                rr[i, :, cols] = value.astype(bf16)

            send(bc, out, i, lambda: (rr.at[i, :, half], rr.at[i, :, half]), there)

        when(bc, body)

    def back3(i, h):
        s = source[i]
        kind, to, out, there, half, mine = routes[h]
        home = ("z0", "z1")[h]

        def body():
            arrive(kind, i, rc.at[i, :, half], to)
            arrive(out, i, rr.at[i, :, half], there)
            if i == 0:
                for j in range(1, planes):
                    arrive(home, source[j], r3.at[source[j], :, half], column[j])

            @pl.loop(0, cut // step)
            def _(n):
                cols, value = merged(i, h, n, lo)
                value = value + rr[i, :, cols].astype(f32)
                if i == 0:
                    for j in range(1, planes):
                        value = value + r3[source[j], :, cols].astype(f32)
                rr[i, :, cols] = value.astype(bf16)

            if i > 0:
                send(ad, home, s, lambda: (rr.at[i, :, half], r3.at[z, :, half]), column[i], got=z)

        when(ad, body)
        if i == 0:
            over = ad & (core != h)
            when(over, lambda: send(over, "dp", h, lambda: (rr.at[0, :, half], out_ref), to_core))

    ops = {
        "sp": spread,
        "gz": lambda i: (gather_z(i, ad), pass_z(i, ad, "tr" if i else "r")),
        "tb": lambda i: (when(ad, table), spread_table(0), pass_z(0, ad, "t")),
        "gi": lambda i: (gather_z(i, ad & inner), pass_z(i, ad & inner)),
        "go": lambda i: gather_z(i, ad & outer),
        "v0": plane_out, "v1": plane_on,
        "za": lambda i: pass_v(i, 0), "zb": lambda i: (diagonal_in(i), pass_v(i, 1)),
        "ra": lambda i: relay_v(i, 0), "rb": lambda i: relay_v(i, 1),
        "sy": share_y, "sx": share_x, "cf": forward,
        "ca": lambda i: backward(i, 0), "cb": lambda i: backward(i, 1),
        "1y": back1_y, "1x": back1_x,
        "2y": lambda i: back2(i, 0), "2x": lambda i: back2(i, 1),
        "3y": lambda i: back3(i, 0), "3x": lambda i: back3(i, 1),
    }
    for name, i in STEPS:
        if name == "cf":
            while loads:
                loads.pop().wait()
        ops[name](i)

    def finish():
        out_ref[...] = jnp.where(core == 0, rr[0, :, 0:cut], rr[0, :, cut:])

    when(ad, finish)
    when(bc, lambda: arrive("dp", core, out_ref, to_core))
    for wait in staged.values():
        wait()
    for cond, wait in sent:
        if cond is None:
            wait()
        else:
            when(cond, wait)


def fused(layer_input, out_grad, expert_ids, gate_probs, gate_proj, up_proj, down_proj):
    experts, halves = lax.axis_size("ep"), lax.axis_size("dp")
    rows, features = layer_input.shape
    hidden = gate_proj.shape[2]
    planes = experts // 4
    cap = capacity(experts, expert_ids.shape)
    cut, bf16, f32 = features // 2, jnp.bfloat16, jnp.float32
    vmem, hbm = pl.BlockSpec(memory_space=pltpu.VMEM), pl.BlockSpec(memory_space=pl.ANY)
    aside = put_aside(features)
    near = (features - aside) // 2
    count = 26 * planes
    return pl.pallas_call(
        functools.partial(kernel, cap),
        name="fused_backward",
        out_shape=jax.ShapeDtypeStruct((rows, cut), bf16),
        in_specs=[hbm] * 7,
        out_specs=vmem,
        scratch_shapes=[
            pltpu.VMEM((planes, 2, rows, 2 * near), bf16),
            pltpu.VMEM((planes, 2, 2, rows, aside), bf16),
            pltpu.VMEM((planes, 2, 2 * experts, rows), f32),
            pltpu.VMEM((2, 2, 2, cap, near), bf16),
            pltpu.VMEM((planes - 1, 2, 2, cap, aside), bf16),
            pltpu.VMEM((planes, 2, 2 * cap, features), bf16),
            pltpu.VMEM((planes, 2 * cap, features), bf16),
            pltpu.VMEM((planes, cap, features), bf16),
            pltpu.VMEM((planes, rows, features), bf16),
            pltpu.VMEM((planes, rows, features), bf16),
            pltpu.VMEM((planes, 2, 2 * cap, rows), bf16),
            pltpu.VMEM((planes, 2, 2, rows, cap), bf16),
            pltpu.VMEM((features, hidden), bf16),
            pltpu.VMEM((features, hidden), bf16),
            pltpu.VMEM((hidden, features), bf16),
            pltpu.VMEM((planes, 2 * cap, hidden), bf16),
            pltpu.VMEM((planes, 2 * cap, hidden), bf16),
            pltpu.VMEM((planes, 2 * cap, 1), f32),
            pltpu.VMEM(expert_ids.shape[::-1], jnp.int32),
            pltpu.VMEM(gate_probs.shape[::-1], f32),
            pltpu.SemaphoreType.DMA((count,)),
            pltpu.SemaphoreType.DMA((count,)),
            pltpu.SemaphoreType.DMA((9,)),
        ],
        compiler_params=pltpu.CompilerParams(
            collective_id=0, has_side_effects=True, vmem_limit_bytes=67043328
        ),
    )(layer_input, out_grad, expert_ids.T, gate_probs.T, gate_proj, up_proj, down_proj)


def put_aside(features):
    return 2 * features // 7 // 256 * 256


def capacity(experts, shape):
    return 5 * shape[0] * shape[1] // (4 * experts)


def dense(layer_input, out_grad, expert_ids, gate_probs, gate_proj, up_proj, down_proj):
    experts = lax.axis_size("ep")
    halves = lax.axis_size("dp")
    tok_rows, features = layer_input.shape
    half = tok_rows // halves
    core = lax.axis_index("dp")
    start = core * half
    mine_in = lax.dynamic_slice_in_dim(layer_input, start, half, 0)
    mine_grad = lax.dynamic_slice_in_dim(out_grad, start, half, 0)
    ids = lax.dynamic_slice_in_dim(expert_ids, start, half, 0)
    probs = lax.dynamic_slice_in_dim(gate_probs, start, half, 0)
    names = jnp.arange(experts, dtype=jnp.int32)
    table = jnp.sum(
        jnp.where(ids[None, :, :] == names[:, None, None], probs[None, :, :], 0.0), axis=2
    )
    weight = lax.all_to_all(table, "ep", split_axis=0, concat_axis=0, tiled=True).reshape(-1)
    in_rows = lax.all_gather(mine_in, "ep", axis=0, tiled=True)
    grad_rows = lax.all_gather(mine_grad, "ep", axis=0, tiled=True)
    gate_mat, up_mat, down_mat = (gate_proj[0], up_proj[0], down_proj[0])
    nt = (((1,), (1,)), ((), ()))
    gate_pre = jnp.dot(in_rows, gate_mat, preferred_element_type=jnp.float32)
    up_pre = jnp.dot(in_rows, up_mat, preferred_element_type=jnp.float32)
    hidden_grad = lax.dot_general(grad_rows, down_mat, nt, preferred_element_type=jnp.float32)
    s = jax.nn.sigmoid(gate_pre)
    gate_grad = (hidden_grad * up_pre * s * (1.0 + gate_pre * (1.0 - s))).astype(jnp.bfloat16)
    up_grad = (hidden_grad * gate_pre * s).astype(jnp.bfloat16)
    back = lax.dot_general(gate_grad, gate_mat, nt, preferred_element_type=jnp.float32)
    back = back + lax.dot_general(up_grad, up_mat, nt, preferred_element_type=jnp.float32)
    back = (back * weight[:, None]).astype(jnp.bfloat16)
    mine = lax.psum_scatter(back, "ep", scatter_dimension=0, tiled=True)
    return lax.all_to_all(mine, "dp", split_axis=1, concat_axis=0, tiled=True)


def body(*args):
    experts, halves = lax.axis_size("ep"), lax.axis_size("dp")
    rows, features = args[0].shape
    hidden = args[4].shape[2]
    cap = capacity(experts, args[2].shape)
    held = 2 * features * (LINE * (4 * rows + 7 * cap) + 3 * hidden + 6 * cap) + 16 * LINE * cap * hidden
    fits = held < 66 * 10**6 and halves == 2 and experts == 4 * LINE and cap % 16 == 0
    return (fused if fits else dense)(*args)


def solution(mesh):
    row = P("ep", None)
    mat = P("ep", None, None)
    return jax.shard_map(
        body, mesh=mesh, in_specs=(row, row, row, row, mat, mat, mat), out_specs=P("ep", "dp"), check_vma=False
    )
```
